32 devices in a mesh: rows: 16 (over z, y, x), feat: 2 (over core).
Axes of the slice: x: 2, y: 2, z: 4, core: 2. Of those that a mesh axis runs over, the one named last changes fastest.
Arguments:
- queries: bfloat16 [1024, 128], P('rows', 'feat'), may hold values from -6 to 6
- corpus: bfloat16 [524288, 128], P(('rows', 'feat')), as said below
- candidates: int32 [1024, 100], P(('rows', 'feat')), may hold values from 0 to 524287, as said below
- threshold: int32 [1024], replicated, may hold values from 100 to 199, as said below
Outputs:
- exceed: float32 [1024], P(('rows', 'feat'))
- candidate_scores: float32 [1024, 100], P(('rows', 'feat'))
The draws below stay inside these ranges and needn't reach their ends.
Inputs may be any that keep to these rules, and one draw needn't show every extreme that they name: Passage ids. Of the 3200 candidates of one device's queries (aligned blocks of 32 rows), at most 100 lie in the 16384 passages of any one device, and exactly 100 in some device's. `corpus`: passage embeddings of order one or smaller; their scale differs between passages. Some query has threshold 100 and some 199.
All inputs are finite; a program needn't handle non-finite values.
Results may differ from the reference program's by a relative error of at most 0.00035.
Values may be sent and summed in bfloat16 or wider, within the bound.
A program may use at most 64 MiB of HBM per device.

```python
import jax
import jax.numpy as jnp
from jax import lax

DIM = 128
NQ = 1024
NCAND = 100
ROWS_DEV = 16384
SHARDS = 32
NPASS = 524288
NQ_DEV = 32


def draw_corpus(key, part):
    blocks_count = NPASS // ROWS_DEV
    block_scale = jnp.exp(jax.random.uniform(jax.random.fold_in(key, 11), (blocks_count,), jnp.float32, jnp.log(0.3), jnp.log(3.0)))
    row_scale = jax.random.uniform(jax.random.fold_in(key, 12), (NPASS,), jnp.float32, 0.7, 1.3)
    base = jax.random.normal(jax.random.fold_in(key, 13), (NPASS, DIM), jnp.float32)
    scale = jnp.repeat(block_scale, ROWS_DEV) * row_scale
    return (base * DIM ** (-0.5) * scale[:, None]).astype(jnp.bfloat16)


def draw_candidates(key, part):
    total = NQ_DEV * NCAND

    def one_source(source):
        source_key = jax.random.fold_in(key, source)
        order = jax.random.permutation(jax.random.fold_in(source_key, 1), total)
        target = order % SHARDS
        offset = jax.random.randint(jax.random.fold_in(source_key, 2), (total,), 0, ROWS_DEV)
        return (target * ROWS_DEV + offset).reshape(NQ_DEV, NCAND)
    sources = jnp.arange(NQ // NQ_DEV, dtype=jnp.int32)
    return jax.vmap(one_source)(sources).reshape(NQ, NCAND).astype(jnp.int32)


def draw_threshold(key, part):
    values = jax.random.randint(jax.random.fold_in(key, 21), (NQ,), 100, 200).astype(jnp.int32)
    order = jax.random.permutation(jax.random.fold_in(key, 22), NQ)
    values = values.at[order[0]].set(100)
    values = values.at[order[1]].set(199)
    return values.astype(jnp.int32)


def block_levels(key, dims, pieces, low, top_value):
    factor_of = 1.0
    for dim, blocks in pieces:
        heights = jax.random.uniform(jax.random.fold_in(jax.random.fold_in(key, 6), dim), (blocks,), jnp.float32, low / len(pieces), top_value / len(pieces))
        factor_of = factor_of * jnp.repeat(jnp.exp(heights), dims[dim] // blocks).reshape((-1,) + (1,) * (len(dims) - 1 - dim))
    return factor_of


def centred(own_key, shape, deviation, reach, shards=(), held_as=jnp.bfloat16):
    result = deviation * jax.random.normal(own_key, shape, jnp.float32)
    if shards:
        result = result * block_levels(own_key, shape, shards, -0.22, 0.18)
    return jnp.clip(result, -reach, reach).astype(held_as)


def setup_inputs(seed: int = 0) -> dict:
    key_list = jax.random.split(jax.random.key(seed), 5)
    queries = centred(key_list[0], (NQ, DIM), 1.0, 6.0, ((0, 16), (1, 2)))
    corpus = draw_corpus(jax.random.fold_in(key_list[4], 71), 0)
    candidates = draw_candidates(jax.random.fold_in(key_list[4], 71), 0)
    threshold = draw_threshold(jax.random.fold_in(key_list[4], 71), 0)
    return {"queries": queries, "corpus": corpus, "candidates": candidates, "threshold": threshold}


def reference(queries, corpus, candidates, threshold):
    cutoff = threshold.astype(jnp.float32) * 0.01
    blocks = corpus.reshape(NPASS // ROWS_DEV, ROWS_DEV, DIM)

    def visit(total, block):
        scores = lax.dot_general(queries, block, (((1,), (1,)), ((), ())), preferred_element_type=jnp.float32)
        return total + jnp.sum(jnp.maximum(scores - cutoff[:, None], 0.0), axis=1), None

    total, _ = lax.scan(visit, jnp.zeros((NQ,), jnp.float32), blocks)
    exceed = total * (8.0 / NPASS)
    flat_ids = candidates.reshape(-1).astype(jnp.int32)
    picked = corpus[flat_ids].astype(jnp.float32).reshape(NQ, NCAND, DIM)
    candidate_scores = jnp.einsum("qkd,qd->qk", picked, queries.astype(jnp.float32), precision=lax.Precision.HIGHEST)
    return exceed, candidate_scores
```

```python
import functools

import jax
import jax.numpy as jnp
from jax import lax
from jax.experimental import pallas as pl
from jax.experimental.pallas import tpu as pltpu
from jax.sharding import PartitionSpec as P

LANES = 128
TILE = 256
ROWS = 256
PIECES = 32
RANGES = 3
LAG = 2
UNITS = (88, 120, 152, 184)
PLAN = {
    0: (("reach", 1),), 40: (("reach", 2),), 48: (("hand", 1),), 72: (("reach", 3),), 96: (("hand", 2),),
    124: (("hand", 3),),
    70: (("ids", 0),), 84: (("sm", 0),), 104: (("ids", 1),), 118: (("sm", 1),),
    136: (("ids", 2),), 150: (("sm", 2),), 168: (("ids", 3),), 182: (("sm", 3),),
    134: (("vals", 0),), 166: (("vals", 1),), 198: (("vals", 2),), 230: (("vals", 3),),
}
MESH = pl.DeviceIdType.MESH


def mark(name):
    pass


def bulk_wait(ref, sem):
    pltpu.make_async_copy(ref, ref, sem).wait()


def kernel(
    n, nf, npass_all, capacity,
    q_hbm, thr_hbm, cand_hbm, corpus_ref,
    mass_hbm, ans_hbm,
    mass_out, ans_out,
    q_ref, thr_ref, cand_ref, corpus_v, corpus_f, q_pack, q_in, q_full, cand_pad, places,
    ids_out, ids_in, ids_at, ids_sm, rows_v, vals_out, vals_in, mass_rows, mass_in,
    small_sem, load_sem, out_sem, sm_sem, in_sem, q_send, q_recv, hand_send, hand_recv,
    ids_send, ids_recv, vals_send, vals_recv, mass_send, mass_recv,
):
    rows_dev, width = corpus_v.shape
    owned, per_query = cand_ref.shape
    nq = q_full.shape[0]
    half = q_ref.shape[1]
    tiles = nq // TILE
    dpt = TILE // owned
    dph = dpt // 2
    chips = n // nf
    dpc = dpt // nf
    core = lax.axis_index("feat")
    me = lax.axis_index("rows") * nf + core
    my_tile = me // dpt
    my_j = me % dpt
    my_half = my_j // dph
    my_h = my_j % dph
    id_bits = rows_dev.bit_length() - 1

    def table(values):
        out = values[0]
        for k in range(1, tiles):
            out = out + (values[k] - values[k - 1]) * ((my_tile + tiles - 1 - k) // (tiles - 1))
        return out

    planes = [my_tile, table((1, 0, 1, 2)), table((2, 2, 0, 1)), table((3, 3, 3, 0))]
    askers = [my_tile, table((1, 0, 1, 2)), table((2, 2, 0, 0)), table((3, 3, 3, 1))]

    load = pltpu.make_async_copy(corpus_ref, corpus_v, load_sem)
    small = [
        pltpu.make_async_copy(src, dst, small_sem.at[k])
        for k, (src, dst) in enumerate(((q_hbm, q_ref), (cand_hbm, cand_ref), (thr_hbm, thr_ref)))]
    for copy in small:
        copy.start()
    load.start()

    def where_is(d):
        return (d // nf, d % nf)

    own_half = [my_tile * dpt + my_half * dph + (my_h + i) % dph for i in range(1, dph)]
    other_half = [my_tile * dpt + (1 - my_half) * dph + (my_h + i) % dph for i in range(dph)]
    neighbours = own_half + other_half

    def plane_of(t):
        return [t * dpt + (my_j + j) % dpt for j in range(dpt)]

    def same_core_of(t):
        return [(t * dpc + (my_j // nf + j) % dpc) * nf + core for j in range(dpc)]

    barrier = pltpu.get_barrier_semaphore()

    def signal(sem, d):
        pl.semaphore_signal(sem, inc=1, device_id=where_is(d), device_id_type=MESH)

    mark("start")
    for d in neighbours:
        signal(barrier, d)
    for k in range(1, tiles):
        @pl.when(my_tile + k < tiles)
        def _():
            for d in plane_of(my_tile + k):
                signal(barrier, d)

    mark("smallwait")
    for copy in small:
        copy.wait()
    mark("pack")
    q_local = q_ref[...].astype(jnp.float32)
    mine = jnp.concatenate([q_local[:owned], q_local[owned:]], axis=1).astype(jnp.bfloat16)
    q_pack[...] = mine
    my_place = core * chips + me // nf
    q_in[my_place] = mine

    mark("barrier")
    pl.semaphore_wait(barrier, dpt - 1 + my_tile * dpt)
    mark("sends1")

    def send_queries(d, sem):
        pltpu.make_async_remote_copy(
            src_ref=q_pack, dst_ref=q_in.at[my_place], send_sem=q_send, recv_sem=sem,
            device_id=where_is(d), device_id_type=MESH).start()

    def send_ids(d):
        pltpu.make_async_remote_copy(
            src_ref=ids_out.at[d], dst_ref=ids_in.at[me], send_sem=ids_send, recv_sem=ids_recv.at[my_tile],
            device_id=where_is(d), device_id_type=MESH).start()

    for d in own_half:
        send_queries(d, q_recv.at[tiles])
    for d in other_half:
        send_queries(d, q_recv.at[tiles + 1])
    for k in range(1, tiles):
        @pl.when(my_tile >= k)
        def _():
            signal(in_sem.at[my_tile], me - k * dpt)
            for d in same_core_of(my_tile - k):
                send_queries(d, q_recv.at[my_tile])

    mark("sort")
    cand_pad[...] = jnp.full(cand_pad.shape, -1, jnp.int32)
    cand_pad[:, :per_query] = cand_ref[...]
    cand = cand_pad[...]
    target = lax.shift_right_arithmetic(cand, jnp.int32(id_bits))
    local = jnp.bitwise_and(cand, jnp.int32(rows_dev - 1))
    low = jnp.bitwise_and(local, jnp.int32(LANES - 1)).astype(jnp.float32)
    high = lax.shift_right_arithmetic(local, jnp.int32(7)).astype(jnp.float32)
    dest = lax.broadcasted_iota(jnp.int32, (n, LANES), 0)
    hot = [jnp.where(target[q:q + 1] == dest, 1.0, 0.0) for q in range(owned)]
    row_i = lax.broadcasted_iota(jnp.int32, (LANES, 2 * LANES), 0)
    col_i = lax.broadcasted_iota(jnp.int32, (LANES, 2 * LANES), 1)
    upper = jnp.where((row_i < col_i) | (col_i >= LANES), 1.0, 0.0).astype(jnp.bfloat16)

    def sort(count0, count1, field0, field1):
        blank = jnp.zeros((TILE, LANES), jnp.bfloat16)
        chunk = TILE // n
        refs = (count0, count1)
        for m in range(2):
            pltpu.matmul_push_rhs(
                jnp.concatenate([upper, jnp.zeros_like(upper)], axis=0), staging_register=0, mxu_index=m)
        for i in range(owned // chunk):
            part = jnp.concatenate(hot[i * chunk:(i + 1) * chunk], axis=0).astype(jnp.bfloat16)
            pltpu.matmul_acc_lhs(
                refs[i % 2][i // 2], jnp.concatenate([part, blank], axis=1),
                load_staged_rhs=0 if i < 2 else None)
        base = jnp.zeros((n, LANES), jnp.float32)
        slot = lax.broadcasted_iota(jnp.int32, (LANES, LANES), 0).astype(jnp.float32)
        fields = []
        for q in range(owned):
            if q % chunk == 0:
                counts = pltpu.matmul_pop(refs[q // chunk % 2][q // chunk // 2])
            block = counts[q % chunk * n:(q % chunk + 1) * n]
            rank = jnp.sum(hot[q] * (block[:, :LANES] + base), axis=0, keepdims=True)
            base = base + block[:, LANES:]
            places[:, q * LANES:(q + 1) * LANES] = jnp.where(rank == slot, 1.0, 0.0).astype(jnp.bfloat16)
            fields.append(jnp.concatenate(
                [hot[q] * low[q:q + 1], hot[q] * high[q:q + 1], hot[q] * float(q)], axis=0
            ).astype(jnp.bfloat16))
        sums = (field0, field1)
        turns = owned // 4
        for i in range(turns):
            pairs = (2 * i, owned // 2 + 2 * i)
            pltpu.matmul_push_rhs(
                jnp.concatenate([places[:, q * LANES:(q + 2) * LANES] for q in pairs], axis=0),
                staging_register=i // 2 % 2, mxu_index=i % 2, transpose=True)
            pltpu.matmul_acc_lhs(
                sums[i % 2],
                jnp.concatenate([jnp.concatenate(fields[q:q + 2], axis=1) for q in pairs], axis=0),
                load_staged_rhs=i // 2 % 2)
        total = pltpu.matmul_pop(field0) + pltpu.matmul_pop(field1)
        sorted_fields = total[:3 * n, :LANES] + total[3 * n:, LANES:]
        packed = (
            sorted_fields[:n] + sorted_fields[n:2 * n] * float(LANES) + sorted_fields[2 * n:] * float(rows_dev)
        ).astype(jnp.int32)
        for t in range(n):
            ids_out[t] = packed[t:t + 1]
        ids_in[me] = ids_out[me]

    pl.run_scoped(
        sort,
        (pltpu.ACC(0)((TILE, TILE), jnp.float32),) * (owned * n // TILE // 2),
        (pltpu.ACC(1)((TILE, TILE), jnp.float32),) * (owned * n // TILE // 2),
        pltpu.ACC(0)((6 * n, TILE), jnp.float32),
        pltpu.ACC(1)((6 * n, TILE), jnp.float32))

    mark("sends2")
    for d in neighbours:
        send_ids(d)
    for k in range(1, tiles):
        @pl.when(my_tile >= k)
        def _():
            for d in plane_of(my_tile - k):
                send_ids(d)

    def reach_up(k):
        @pl.when(my_tile + k < tiles)
        def _():
            pl.semaphore_wait(in_sem.at[my_tile + k], 1)
            for d in same_core_of(my_tile + k):
                send_queries(d, q_recv.at[my_tile])
            for d in plane_of(my_tile + k):
                send_ids(d)

    def hand_over(p):
        blocks_of = q_in.at[pl.ds(core * chips + planes[p] * dpc, dpc)]
        bulk_wait(blocks_of, q_recv.at[planes[p]])
        pltpu.make_async_remote_copy(
            src_ref=blocks_of, dst_ref=blocks_of, send_sem=hand_send, recv_sem=hand_recv.at[planes[p]],
            device_id=where_is(me + 1 - 2 * core), device_id_type=MESH).start()

    left = lax.broadcasted_iota(jnp.int32, (owned, LANES), 1) < half

    def unpack(chip):
        f0 = q_in[chip].astype(jnp.float32)
        f1 = q_in[chips + chip].astype(jnp.float32)
        both = jnp.concatenate(
            [jnp.where(left, f0, pltpu.roll(f1, half, 1)), jnp.where(left, pltpu.roll(f0, half, 1), f1)], axis=0)
        q_full[pl.ds(pl.multiple_of(chip * 2 * owned, 2 * owned), 2 * owned), :] = both.astype(jnp.bfloat16)

    order = [(0, None), (0, None), (1, 0), (1, 1), (2, 0), (3, 0), (3, 1), (2, 1)]

    def arrive(b):
        p, side = order[b]
        if b == 0:
            bulk_wait(q_in.at[pl.ds(0, dph - 1)], q_recv.at[tiles])
            first, many = my_tile * dpc + my_half * (dpc // 2), dpc // 2
        elif b == 1:
            bulk_wait(q_in.at[pl.ds(0, dph)], q_recv.at[tiles + 1])
            first, many = my_tile * dpc + (1 - my_half) * (dpc // 2), dpc // 2
        elif side == 0:
            bulk_wait(q_in.at[pl.ds(0, dpc)], hand_recv.at[planes[p]])
            first, many = planes[p] * dpc, dpc
        else:
            many = 0
        for g in range(many):
            unpack(first + g)

    def block_of(b):
        p, side = order[b]
        if b == 0:
            return my_tile * 2 + my_half
        if b == 1:
            return my_tile * 2 + 1 - my_half
        return planes[p] * 2 + side

    def stage_ids(u):
        take = dpt - 1 if u == 0 else dpt
        bulk_wait(ids_in.at[pl.ds(0, take)], ids_recv.at[askers[u]])
        ids_at[pl.ds(u * dpt, dpt)] = jnp.bitwise_and(
            ids_in[pl.ds(pl.multiple_of(askers[u] * dpt, dpt), dpt)], jnp.int32(rows_dev - 1))
        to_smem(u).start()

    def to_smem(u):
        at = pl.ds(u * dpt, dpt)
        return pltpu.make_async_copy(ids_at.at[at], ids_sm.at[at], sm_sem.at[u])

    def send_vals(u):
        if u == 0:
            vals_in[me] = vals_out[my_j]
        for j in range(1 if u == 0 else 0, dpt):
            at = (my_j + j) % dpt
            pltpu.make_async_remote_copy(
                src_ref=vals_out.at[u * dpt + at], dst_ref=vals_in.at[me], send_sem=vals_send, recv_sem=vals_recv,
                device_id=where_is(askers[u] * dpt + at), device_id_type=MESH).start()

    who_q = lax.broadcasted_iota(jnp.int32, (owned, LANES), 0)
    in_use = lax.broadcasted_iota(jnp.int32, (owned, LANES), 1) < capacity
    zeros = jnp.zeros((LANES, LANES), jnp.bfloat16)

    def diagonal(a, b):
        z = zeros[:a.shape[0]]
        return jnp.concatenate([jnp.concatenate([a, z], axis=1), jnp.concatenate([z, b], axis=1)], axis=0)

    def stream(*accs):
        ranges = (accs[:RANGES], accs[RANGES:2 * RANGES])
        extra = accs[2 * RANGES:]
        turn = [0, 0]
        staged = [[], []]
        pending = []
        sums = {}
        count = [0, 0]

        def push(m, value):
            r = turn[m]
            turn[m] = 1 - r
            pltpu.matmul_push_rhs(value, staging_register=r, mxu_index=m, transpose=True)
            staged[m].append(r)
            assert len(staged[m]) <= 2

        def weights(b):
            at = block_of(b)
            q = q_full[pl.ds(pl.multiple_of(at * LANES, LANES), LANES), :]
            return diagonal(q, q)

        def pop():
            kind, m, ref, data = pending.pop(0)
            got = pltpu.matmul_pop(ref)
            if kind == "sweep":
                over = jnp.maximum(got - data[1], 0.0).reshape(ROWS // 16, 2, 8, 2 * LANES)
                part = jnp.sum(over, axis=0)
                sums[data[0]] = sums[data[0]] + part if data[0] in sums else part
            else:
                u, a = data
                for e in range(2):
                    j = 2 * a + e
                    who = lax.shift_right_arithmetic(
                        ids_in[askers[u] * dpt + j], jnp.int32(id_bits))
                    picked = jnp.where((who == who_q) & in_use, got[:, e * LANES:(e + 1) * LANES], 0.0)
                    vals_out[u * dpt + j] = jnp.sum(picked, axis=0, keepdims=True)

        def drain(depth):
            while len(pending) > depth:
                pop()

        def finish(b):
            acc = sums.pop(b)
            acc = acc[0] + acc[1]
            acc = acc[:, :LANES] + acc[:, LANES:]
            at = block_of(b)
            mass_rows[b] = jnp.sum(acc, axis=0, keepdims=True)
            if b == 0:
                mass_in[me] = mass_rows[b]
                dests = own_half
            else:
                dests = [at * dph + (my_h + i) % dph for i in range(dph)]
            for d in dests:
                pltpu.make_async_remote_copy(
                    src_ref=mass_rows.at[b], dst_ref=mass_in.at[me],
                    send_sem=mass_send, recv_sem=mass_recv,
                    device_id=where_is(d), device_id_type=MESH).start()

        def gather(u, k):
            j, r = k // capacity, k % capacity
            rows_v[u * dpt + j, pl.ds(r, 1), :] = corpus_f[pl.ds(ids_sm[u * dpt + j, 0, r], 1), :]

        def widen(k):
            size = rows_dev // (2 * PIECES)
            at = pl.ds(k * size, size)
            corpus_f[at, :] = corpus_v[at, :].astype(jnp.float32)

        def ask(u, a):
            m = a % 2
            at = u * dpt + 2 * a
            push(m, diagonal(rows_v[at].astype(jnp.bfloat16), rows_v[at + 1].astype(jnp.bfloat16)))
            push(m, current[0])

        def reply(u, a):
            m = a % 2
            first = askers[u] * dpt + 2 * a
            q = q_full[pl.ds(pl.multiple_of(first * owned, 2 * owned), 2 * owned), :]
            pltpu.matmul_acc_lhs(
                extra[m], jnp.concatenate([q[:owned], q[owned:]], axis=1), load_staged_rhs=staged[m].pop(0))
            pending.append(("pair", m, extra[m], (u, a)))

        current = [None]
        acts = dict(reach=reach_up, hand=hand_over, ids=stage_ids, sm=lambda u: to_smem(u).wait(), vals=send_vals)
        gathers, asks, replies, reload = {}, {}, {}, set()
        per_step = 2 * dpt * capacity // (2 * PIECES)
        for u, s0 in enumerate(UNITS):
            for i in range(PIECES):
                gathers[s0 + i] = (u, i * per_step, (i + 1) * per_step)
            for a in range(dpt // 2):
                s1 = s0 + (a + 1) * PIECES * 2 // dpt + 1
                asks[s1] = (u, a)
                s1 += 6
                s1 += (s1 + a) % 2
                replies[s1] = (u, a)
                reload.add(s1)

        for b in range(2 * tiles):
            cut = None
            for piece in range(PIECES):
                step = b * PIECES + piece
                for name, arg in PLAN.get(step, ()):
                    mark(f"{name}{arg}")
                    acts[name](arg)
                    mark(f"go{step}")
                if piece == 0:
                    mark(f"arrive{b}")
                    arrive(b)
                    if b == 0:
                        load.wait()
                    mark(f"block{b}")
                    current[0] = weights(b)
                    for m in range(2):
                        push(m, current[0])
                    cut = thr_ref[:, pl.ds(pl.multiple_of(block_of(b) * LANES, LANES), LANES)].astype(jnp.float32) * 0.01
                    cut = jnp.concatenate([cut, cut], axis=1)
                m = piece % 2
                if step in replies:
                    reply(*replies[step])
                at = pl.ds(piece * ROWS, ROWS)
                lhs = jnp.concatenate(
                    [corpus_v[at, :], corpus_v[pl.ds(rows_dev // 2 + piece * ROWS, ROWS), :]], axis=1)
                ref = ranges[m][count[m] % RANGES]
                count[m] += 1
                pltpu.matmul_acc_lhs(ref, lhs, load_staged_rhs=staged[m].pop(0) if piece < 2 or step in reload else None)
                pending.append(("sweep", m, ref, (b, cut)))
                if step in asks:
                    ask(*asks[step])
                if step in gathers:
                    u, k0, k1 = gathers[step]
                    for k in range(k0, k1):
                        gather(u, k)
                if step < 2 * PIECES:
                    widen(step)
                drain(2 * LAG)
                if piece == 2 * LAG - 1 and b > 0:
                    finish(b - 1)
        drain(0)
        finish(2 * tiles - 1)

    pl.run_scoped(
        stream,
        *[pltpu.ACC(0)((ROWS, TILE), jnp.float32)] * RANGES,
        *[pltpu.ACC(1)((ROWS, TILE), jnp.float32)] * RANGES,
        pltpu.ACC(0)((owned, TILE), jnp.float32),
        pltpu.ACC(1)((owned, TILE), jnp.float32))

    mark("valswait")
    bulk_wait(vals_in.at[pl.ds(0, n - 1)], vals_recv)
    mark("spread")
    values = jnp.concatenate([vals_in[t] for t in range(n)], axis=0)
    top = values.astype(jnp.bfloat16)
    rest = values - top.astype(jnp.float32)
    mid = rest.astype(jnp.bfloat16)
    last = (rest - mid.astype(jnp.float32)).astype(jnp.bfloat16)
    upper_part = jnp.concatenate([top, mid], axis=1)
    lower_part = jnp.concatenate([last, jnp.zeros_like(last)], axis=1)
    cand = cand_pad[...]
    target = lax.shift_right_arithmetic(cand, jnp.int32(id_bits))
    dest = lax.broadcasted_iota(jnp.int32, (n, LANES), 0)

    def spread(*refs):
        for i in range(owned // 2):
            place = places[:, 2 * i * LANES:2 * (i + 1) * LANES]
            pltpu.matmul_push_rhs(
                jnp.concatenate([place, place], axis=0), staging_register=i // 2 % 2, mxu_index=i % 2)
            pltpu.matmul_acc_lhs(refs[i % 2][i // 2], upper_part, load_staged_rhs=i // 2 % 2)
            pltpu.matmul_acc_lhs(refs[i % 2][i // 2], lower_part)
        for i in range(owned // 2):
            both = pltpu.matmul_pop(refs[i % 2][i // 2])
            for e in range(2):
                q = 2 * i + e
                ans_out[q:q + 1, :] = jnp.sum(
                    jnp.where(target[q:q + 1] == dest, both[:, e * LANES:(e + 1) * LANES], 0.0),
                    axis=0, keepdims=True)[:, :per_query]

    pl.run_scoped(
        spread,
        (pltpu.ACC(0)((n, TILE), jnp.float32),) * (owned // 4),
        (pltpu.ACC(1)((n, TILE), jnp.float32),) * (owned // 4))

    store_ans = pltpu.make_async_copy(ans_out, ans_hbm, out_sem.at[0])
    store_ans.start()
    mark("masswait")
    bulk_wait(mass_in.at[pl.ds(0, n - 1)], mass_recv)
    mark("masssum")
    mass = mass_in[0]
    for t in range(1, n):
        mass = mass + mass_in[t]
    mass = mass * (8.0 / npass_all)
    per_row = LANES // owned
    result = mass
    for u in range(1, per_row):
        result = jnp.where(me % per_row == u, pltpu.roll(mass, LANES - u * owned, 1), result)
    mass_out[...] = result[:, :owned]
    store_mass = pltpu.make_async_copy(mass_out, mass_hbm, out_sem.at[1])
    store_mass.start()

    mark("sendwaits")
    bulk_wait(q_in.at[pl.ds(0, dpt - 1 + (tiles - 1) * dpc)], q_send)
    bulk_wait(q_in.at[pl.ds(0, (tiles - 1) * dpc)], hand_send)
    bulk_wait(ids_in.at[pl.ds(0, n - 1)], ids_send)
    bulk_wait(vals_in.at[pl.ds(0, n - 1)], vals_send)
    bulk_wait(mass_in.at[pl.ds(0, n - 1)], mass_send)
    store_ans.wait()
    store_mass.wait()
    mark(None)


def fused_body(n, nf, queries, corpus, candidates, threshold):
    rows_dev, width = corpus.shape
    owned, per_query = candidates.shape
    nq = n * owned
    tiles = nq // TILE
    capacity = (owned * per_query + n - 1) // n
    mass, answers = pl.pallas_call(
        functools.partial(kernel, n, nf, rows_dev * n, capacity),
        out_shape=(
            jax.ShapeDtypeStruct((1, owned), jnp.float32),
            jax.ShapeDtypeStruct((owned, per_query), jnp.float32),
        ),
        in_specs=[pl.BlockSpec(memory_space=pl.ANY)] * 4,
        out_specs=[pl.BlockSpec(memory_space=pl.ANY)] * 2,
        scratch_shapes=[
            pltpu.VMEM((1, owned), jnp.float32),
            pltpu.VMEM((owned, per_query), jnp.float32),
            pltpu.VMEM(queries.shape, jnp.bfloat16),
            pltpu.VMEM((1, nq), jnp.int32),
            pltpu.VMEM((owned, per_query), jnp.int32),
            pltpu.VMEM((rows_dev, width), jnp.bfloat16),
            pltpu.VMEM((rows_dev, width), jnp.float32),
            pltpu.VMEM((owned, LANES), jnp.bfloat16),
            pltpu.VMEM((n, owned, LANES), jnp.bfloat16),
            pltpu.VMEM((nq, LANES), jnp.bfloat16),
            pltpu.VMEM((owned, LANES), jnp.int32),
            pltpu.VMEM((LANES, owned * LANES), jnp.bfloat16),
            pltpu.VMEM((n, 1, LANES), jnp.int32),
            pltpu.VMEM((n, 1, LANES), jnp.int32),
            pltpu.VMEM((n, 1, LANES), jnp.int32),
            pltpu.SMEM((n, 1, LANES), jnp.int32),
            pltpu.VMEM((n, LANES, LANES), jnp.float32),
            pltpu.VMEM((n, 1, LANES), jnp.float32),
            pltpu.VMEM((n, 1, LANES), jnp.float32),
            pltpu.VMEM((nq // LANES, 1, LANES), jnp.float32),
            pltpu.VMEM((n, 1, LANES), jnp.float32),
            pltpu.SemaphoreType.DMA((3,)),
            pltpu.SemaphoreType.DMA,
            pltpu.SemaphoreType.DMA((2,)),
            pltpu.SemaphoreType.DMA((tiles,)),
            pltpu.SemaphoreType.REGULAR((tiles,)),
            pltpu.SemaphoreType.DMA,
            pltpu.SemaphoreType.DMA((tiles + 2,)),
            pltpu.SemaphoreType.DMA,
            pltpu.SemaphoreType.DMA((tiles,)),
            pltpu.SemaphoreType.DMA,
            pltpu.SemaphoreType.DMA((tiles,)),
            pltpu.SemaphoreType.DMA,
            pltpu.SemaphoreType.DMA,
            pltpu.SemaphoreType.DMA,
            pltpu.SemaphoreType.DMA,
        ],
        compiler_params=pltpu.CompilerParams(
            collective_id=0, has_side_effects=True),
    )(queries, threshold.reshape(1, nq), candidates, corpus)
    return mass.reshape(owned), answers


def plain_body(queries, corpus, candidates, threshold):
    rows_dev = corpus.shape[0]
    width = corpus.shape[1]
    shards = lax.axis_size("rows") * lax.axis_size("feat")
    owned_queries = candidates.shape[0]
    per_query = candidates.shape[1]
    npass_all = rows_dev * shards
    cutoff = threshold.astype(jnp.float32) * 0.01
    owner = lax.axis_index(("rows", "feat"))
    full_rows = lax.all_gather(queries, "feat", axis=1, tiled=True)
    whole = lax.all_gather(full_rows, "rows", axis=0, tiled=True)
    query_count = whole.shape[0]
    block = 2048
    corpus_blocks = corpus.reshape(rows_dev // block, block, width)

    def visit(total, block_rows):
        scores = lax.dot_general(
            whole, block_rows, (((1,), (1,)), ((), ())), preferred_element_type=jnp.float32
        )
        return (total + jnp.sum(jnp.maximum(scores - cutoff[:, None], 0.0), axis=1), None)

    total, _ = lax.scan(visit, jnp.zeros((query_count,), jnp.float32), corpus_blocks)
    flat_ids = candidates.reshape(-1)
    total_ids = flat_ids.shape[0]
    capacity = (total_ids + shards - 1) // shards
    target = flat_ids // rows_dev
    onehot = (target[:, None] == jnp.arange(shards, dtype=jnp.int32)[None, :]).astype(jnp.int32)
    before = jnp.cumsum(onehot, axis=0) - onehot
    rank = jnp.sum(before * onehot, axis=1)
    query_ids = owner * owned_queries + jnp.arange(total_ids, dtype=jnp.int32) // per_query
    fields = jnp.stack([flat_ids - target * rows_dev, query_ids], axis=1)
    send_both = jnp.zeros((shards, capacity, 2), jnp.int32).at[target, rank].set(fields)
    n_rows = lax.axis_size("rows")
    n_feat = lax.axis_size("feat")
    received = lax.all_to_all(
        lax.all_to_all(
            send_both.reshape(n_rows, n_feat, capacity * 2),
            "rows",
            split_axis=0,
            concat_axis=0,
            tiled=True,
        ),
        "feat",
        split_axis=1,
        concat_axis=1,
        tiled=True,
    )
    received = received.reshape(shards * capacity, 2)
    picked = corpus[received[:, 0]]
    asked = whole[received[:, 1]]
    values = jnp.einsum("kd,kd->k", picked, asked, preferred_element_type=jnp.float32).reshape(
        n_rows, n_feat, capacity
    )
    partials = total.reshape(n_rows, n_feat, owned_queries)
    answers, mass_parts = (
        lax.all_to_all(
            lax.all_to_all(values, "rows", split_axis=0, concat_axis=0, tiled=True),
            "feat",
            split_axis=1,
            concat_axis=1,
            tiled=True,
        ),
        lax.all_to_all(
            lax.all_to_all(partials, "rows", split_axis=0, concat_axis=0, tiled=True),
            "feat",
            split_axis=1,
            concat_axis=1,
            tiled=True,
        ),
    )
    exceed = jnp.sum(mass_parts, axis=(0, 1)) * (8.0 / npass_all)
    candidate_scores = answers.reshape(shards, capacity)[target, rank].reshape(
        owned_queries, per_query
    )
    return (exceed, candidate_scores)


def body(queries, corpus, candidates, threshold):
    nf = lax.axis_size("feat")
    n = lax.axis_size("rows") * nf
    rows_dev, width = corpus.shape
    owned, per_query = candidates.shape
    capacity = (owned * per_query + n - 1) // n
    fits = (
        nf == 2
        and width == LANES
        and queries.shape == (2 * owned, LANES // 2)
        and owned % 32 == 0
        and LANES % owned == 0
        and per_query <= LANES
        and capacity <= LANES
        and n % 8 == 0
        and (n * owned) % TILE == 0
        and n * owned == 4 * TILE
        and rows_dev == 2 * ROWS * PIECES
        and rows_dev & (rows_dev - 1) == 0
    )
    if fits:
        return fused_body(n, nf, queries, corpus, candidates, threshold)
    return plain_body(queries, corpus, candidates, threshold)


def solution(mesh):
    return jax.shard_map(
        body,
        mesh=mesh,
        in_specs=(P("rows", "feat"), P(("rows", "feat"), None), P(("rows", "feat"), None), P()),
        out_specs=(P(("rows", "feat")), P(("rows", "feat"), None)),
        check_vma=False,
    )
```

```python
import functools

import jax
import jax.numpy as jnp
from jax import lax
from jax.experimental import pallas as pl
from jax.experimental.pallas import tpu as pltpu
from jax.sharding import PartitionSpec as P

LANES = 128
TILE = 256
ROWS = 256
PIECES = 32
RANGES = 3
LAG = 2
AHEAD = 5
UNITS = {
    0: (74, 32, (96, 112)), 1: (108, 16, (128, 144)), 2: (154, 32, (176, 192)), 3: (186, 32, (208, 224)),
}
PLAN = {
    20: (("arrive", 1),),
    38: (("mass", 0), ("reach", 2), ("hand", 1)),
    54: (("reach", 3), ("ids", 0)),
    58: (("arrive", 2),),
    70: (("mass", 1), ("sm", 0)),
    100: (("ids", 1), ("hand", 2)),
    106: (("mass", 2), ("sm", 1)),
    118: (("vals", 0),),
    122: (("arrive", 4),),
    134: (("mass", 3), ("ids", 2)),
    150: (("vals", 1), ("hand", 3), ("sm", 2)),
    166: (("mass", 4), ("ids", 3)),
    172: (("arrive", 6),),
    182: (("sm", 3),),
    198: (("mass", 5), ("vals", 2)),
    230: (("mass", 6), ("vals", 3)),
}
FENCES = frozenset(range(0, 224, 8))
LOGICAL = pl.DeviceIdType.LOGICAL


def mark(name):
    pass


def bulk_wait(ref, sem):
    pltpu.make_async_copy(ref, ref, sem).wait()


def kernel(
    n, nf, npass_all, capacity,
    q_hbm, thr_hbm, cand_hbm, corpus_ref,
    mass_out, ans_out,
    q_ref, thr_ref, cand_ref, corpus_v, corpus_f, q_pack, q_in, q_full, cand_pad, places,
    ids_out, ids_in, ids_at, ids_sm, rows_v, vals_out, vals_in, mass_rows, mass_in,
    small_sem, load_sem, sm_sem, in_sem, fence_sem, q_send, q_recv, hand_send, hand_recv,
    ids_send, ids_recv, vals_send, vals_recv, mass_send, mass_recv,
):
    rows_dev, width = corpus_v.shape
    owned, per_query = cand_ref.shape
    nq = q_full.shape[0]
    half = q_ref.shape[1]
    tiles = nq // TILE
    dpt = TILE // owned
    dph = dpt // 2
    chips = n // nf
    dpc = dpt // nf
    core = lax.axis_index("feat")
    me = lax.axis_index("rows") * nf + core
    my_tile = me // dpt
    my_j = me % dpt
    my_half = my_j // dph
    my_h = my_j % dph
    id_bits = rows_dev.bit_length() - 1

    def table(values):
        out = values[0]
        for k in range(1, tiles):
            out = out + (values[k] - values[k - 1]) * ((my_tile + tiles - 1 - k) // (tiles - 1))
        return out

    planes = [my_tile, table((1, 0, 1, 2)), table((2, 2, 0, 0)), table((3, 3, 3, 1))]
    askers = planes[1:] + planes[:1]

    load = pltpu.make_async_copy(corpus_ref, corpus_v, load_sem)
    small = [
        pltpu.make_async_copy(src, dst, small_sem.at[k])
        for k, (src, dst) in enumerate(((q_hbm, q_ref), (cand_hbm, cand_ref), (thr_hbm, thr_ref)))]
    for copy in small:
        copy.start()
    load.start()

    around = [(my_h + i) % dph for i in range(dph)]
    own_half = [my_tile * dpt + my_half * dph + j for j in around[1:]]
    other_half = [my_tile * dpt + (1 - my_half) * dph + j for j in around]
    neighbours = own_half + other_half

    def plane_of(t):
        return [t * dpt + (my_j + j) % dpt for j in range(dpt)]

    def same_core_of(t):
        return [(t * dpc + (my_j // nf + j) % dpc) * nf + core for j in range(dpc)]

    barrier = pltpu.get_barrier_semaphore()

    def signal(sem, d):
        pl.semaphore_signal(sem, inc=1, device_id=(d), device_id_type=LOGICAL)

    mark("start")
    for d in neighbours:
        signal(barrier, d)
    for k in range(1, tiles):
        @pl.when(my_tile + k < tiles)
        def _():
            for d in plane_of(my_tile + k):
                signal(barrier, d)

    mark("smallwait")
    for copy in small:
        copy.wait()
    mark("pack")
    q_local = q_ref[...].astype(jnp.float32)
    mine = jnp.concatenate([q_local[:owned], q_local[owned:]], axis=1).astype(jnp.bfloat16)
    q_pack[...] = mine
    my_place = core * chips + me // nf
    q_in[my_place] = mine

    mark("barrier")
    pl.semaphore_wait(barrier, dpt - 1 + my_tile * dpt)
    mark("sends1")

    def send_queries(d, sem):
        pltpu.make_async_remote_copy(
            src_ref=q_pack, dst_ref=q_in.at[my_place], send_sem=q_send, recv_sem=sem,
            device_id=(d), device_id_type=LOGICAL).start()

    def send_ids(d):
        pltpu.make_async_remote_copy(
            src_ref=ids_out.at[d], dst_ref=ids_in.at[me], send_sem=ids_send, recv_sem=ids_recv.at[my_tile],
            device_id=(d), device_id_type=LOGICAL).start()

    for d in own_half:
        send_queries(d, q_recv.at[tiles])
    for d in other_half:
        send_queries(d, q_recv.at[tiles + 1])
    for k in range(1, tiles):
        @pl.when(my_tile >= k)
        def _():
            signal(in_sem.at[my_tile], me - k * dpt)
            for d in same_core_of(my_tile - k):
                send_queries(d, q_recv.at[my_tile])

    mark("sort")
    cand_pad[...] = jnp.full(cand_pad.shape, -1, jnp.int32)
    cand_pad[:, :per_query] = cand_ref[...]
    cand = cand_pad[...]
    target = lax.shift_right_arithmetic(cand, jnp.int32(id_bits))
    local = jnp.bitwise_and(cand, jnp.int32(rows_dev - 1))
    low = jnp.bitwise_and(local, jnp.int32(LANES - 1)).astype(jnp.float32)
    high = lax.shift_right_arithmetic(local, jnp.int32(7)).astype(jnp.float32)
    dest = lax.broadcasted_iota(jnp.int32, (n, LANES), 0)
    hot = [jnp.where(target[q:q + 1] == dest, 1.0, 0.0) for q in range(owned)]
    row_i = lax.broadcasted_iota(jnp.int32, (LANES, 2 * LANES), 0)
    col_i = lax.broadcasted_iota(jnp.int32, (LANES, 2 * LANES), 1)
    upper = jnp.where((row_i < col_i) | (col_i >= LANES), 1.0, 0.0).astype(jnp.bfloat16)

    def sort(count0, count1, field0, field1):
        blank = jnp.zeros((TILE, LANES), jnp.bfloat16)
        chunk = TILE // n
        refs = (count0, count1)
        for m in range(2):
            pltpu.matmul_push_rhs(
                jnp.concatenate([upper, jnp.zeros_like(upper)], axis=0), staging_register=0, mxu_index=m)
        for i in range(owned // chunk):
            part = jnp.concatenate(hot[i * chunk:(i + 1) * chunk], axis=0).astype(jnp.bfloat16)
            pltpu.matmul_acc_lhs(
                refs[i % 2][i // 2], jnp.concatenate([part, blank], axis=1),
                load_staged_rhs=0 if i < 2 else None)
        base = jnp.zeros((n, LANES), jnp.float32)
        slot = lax.broadcasted_iota(jnp.int32, (LANES, LANES), 0).astype(jnp.float32)
        fields = []
        for q in range(owned):
            if q % chunk == 0:
                counts = pltpu.matmul_pop(refs[q // chunk % 2][q // chunk // 2])
            block = counts[q % chunk * n:(q % chunk + 1) * n]
            rank = jnp.sum(hot[q] * (block[:, :LANES] + base), axis=0, keepdims=True)
            base = base + block[:, LANES:]
            places[:, q * LANES:(q + 1) * LANES] = jnp.where(rank == slot, 1.0, 0.0).astype(jnp.bfloat16)
            fields.append(jnp.concatenate(
                [hot[q] * low[q:q + 1], hot[q] * high[q:q + 1], hot[q] * float(q)], axis=0
            ).astype(jnp.bfloat16))
        sums = (field0, field1)
        turns = owned // 4
        for i in range(turns):
            pairs = (2 * i, owned // 2 + 2 * i)
            pltpu.matmul_push_rhs(
                jnp.concatenate([places[:, q * LANES:(q + 2) * LANES] for q in pairs], axis=0),
                staging_register=i // 2 % 2, mxu_index=i % 2, transpose=True)
            pltpu.matmul_acc_lhs(
                sums[i % 2],
                jnp.concatenate([jnp.concatenate(fields[q:q + 2], axis=1) for q in pairs], axis=0),
                load_staged_rhs=i // 2 % 2)
        total = pltpu.matmul_pop(field0) + pltpu.matmul_pop(field1)
        sorted_fields = total[:3 * n, :LANES] + total[3 * n:, LANES:]
        packed = (
            sorted_fields[:n] + sorted_fields[n:2 * n] * float(LANES) + sorted_fields[2 * n:] * float(rows_dev)
        ).astype(jnp.int32)
        for t in range(n):
            ids_out[t] = packed[t:t + 1]
        ids_in[me] = ids_out[me]

    pl.run_scoped(
        sort,
        (pltpu.ACC(0)((TILE, TILE), jnp.float32),) * (owned * n // TILE // 2),
        (pltpu.ACC(1)((TILE, TILE), jnp.float32),) * (owned * n // TILE // 2),
        pltpu.ACC(0)((6 * n, TILE), jnp.float32),
        pltpu.ACC(1)((6 * n, TILE), jnp.float32))

    mark("sends2")
    for d in neighbours:
        send_ids(d)
    for k in range(1, tiles):
        @pl.when(my_tile >= k)
        def _():
            for d in plane_of(my_tile - k):
                send_ids(d)

    def reach_up(k):
        @pl.when(my_tile + k < tiles)
        def _():
            pl.semaphore_wait(in_sem.at[my_tile + k], 1)
            for d in same_core_of(my_tile + k):
                send_queries(d, q_recv.at[my_tile])
            for d in plane_of(my_tile + k):
                send_ids(d)

    def hand_over(p):
        blocks_of = q_in.at[pl.ds(core * chips + planes[p] * dpc, dpc)]
        bulk_wait(blocks_of, q_recv.at[planes[p]])
        pltpu.make_async_remote_copy(
            src_ref=blocks_of, dst_ref=blocks_of, send_sem=hand_send, recv_sem=hand_recv.at[planes[p]],
            device_id=(me + 1 - 2 * core), device_id_type=LOGICAL).start()

    left = lax.broadcasted_iota(jnp.int32, (owned, LANES), 1) < half

    def unpack(chip):
        f0 = q_in[chip].astype(jnp.float32)
        f1 = q_in[chips + chip].astype(jnp.float32)
        both = jnp.concatenate(
            [jnp.where(left, f0, pltpu.roll(f1, half, 1)), jnp.where(left, pltpu.roll(f0, half, 1), f1)], axis=0)
        q_full[pl.ds(pl.multiple_of(chip * 2 * owned, 2 * owned), 2 * owned), :] = both.astype(jnp.bfloat16)

    order = [(b // 2, b % 2) for b in range(2 * tiles)]

    def arrive(b):
        p, side = order[b]
        if b == 0:
            bulk_wait(q_in.at[pl.ds(0, dph - 1)], q_recv.at[tiles])
            first, many = my_tile * dpc + my_half * (dpc // 2), dpc // 2
        elif b == 1:
            bulk_wait(q_in.at[pl.ds(0, dph)], q_recv.at[tiles + 1])
            first, many = my_tile * dpc + (1 - my_half) * (dpc // 2), dpc // 2
        elif side == 0:
            bulk_wait(q_in.at[pl.ds(0, dpc)], hand_recv.at[planes[p]])
            first, many = planes[p] * dpc, dpc
        else:
            many = 0
        for g in range(many):
            unpack(first + g)

    def block_of(b):
        p, side = order[b]
        if b == 0:
            return my_tile * 2 + my_half
        if b == 1:
            return my_tile * 2 + 1 - my_half
        return planes[p] * 2 + side

    def stage_ids(u):
        take = dpt - 1 if u == tiles - 1 else dpt
        bulk_wait(ids_in.at[pl.ds(0, take)], ids_recv.at[askers[u]])
        ids_at[pl.ds(u * dpt, dpt)] = jnp.bitwise_and(
            ids_in[pl.ds(pl.multiple_of(askers[u] * dpt, dpt), dpt)], jnp.int32(rows_dev - 1))
        to_smem(u).start()

    def to_smem(u):
        at = pl.ds(u * dpt, dpt)
        return pltpu.make_async_copy(ids_at.at[at], ids_sm.at[at], sm_sem.at[u])

    def send_vals(u):
        if u == tiles - 1:
            vals_in[me] = vals_out[u * dpt + my_j]
        for j in range(1 if u == tiles - 1 else 0, dpt):
            at = (my_j + j) % dpt
            pltpu.make_async_remote_copy(
                src_ref=vals_out.at[u * dpt + at], dst_ref=vals_in.at[me], send_sem=vals_send, recv_sem=vals_recv,
                device_id=(askers[u] * dpt + at), device_id_type=LOGICAL).start()

    who_q = lax.broadcasted_iota(jnp.int32, (owned, LANES), 0)
    in_use = lax.broadcasted_iota(jnp.int32, (owned, LANES), 1) < capacity
    zeros = jnp.zeros((LANES, LANES), jnp.bfloat16)

    def diagonal(a, b):
        z = zeros[:a.shape[0]]
        return jnp.concatenate([jnp.concatenate([a, z], axis=1), jnp.concatenate([z, b], axis=1)], axis=0)

    def stream(*accs):
        ranges = (accs[:RANGES], accs[RANGES:2 * RANGES])
        extra = accs[2 * RANGES:]
        turn = [0, 0]
        staged = [[], []]
        pending = []
        sums = {}
        count = [0, 0]

        def push(m, value):
            r = turn[m]
            turn[m] = 1 - r
            pltpu.matmul_push_rhs(value, staging_register=r, mxu_index=m, transpose=True)
            staged[m].append(r)
            assert len(staged[m]) <= 2

        def weights(b):
            at = block_of(b)
            q = q_full[pl.ds(pl.multiple_of(at * LANES, LANES), LANES), :]
            return diagonal(q, q)

        def pop():
            kind, m, ref, data = pending.pop(0)
            got = pltpu.matmul_pop(ref)
            if kind == "sweep":
                over = jnp.maximum(got - data[1], 0.0).reshape(ROWS // 16, 2, 8, 2 * LANES)
                part = jnp.sum(over, axis=0)
                sums[data[0]] = sums[data[0]] + part if data[0] in sums else part
            else:
                u, a = data
                for e in range(2):
                    j = 2 * a + e
                    who = lax.shift_right_arithmetic(
                        ids_in[askers[u] * dpt + j], jnp.int32(id_bits))
                    picked = jnp.where((who == who_q) & in_use, got[:, e * LANES:(e + 1) * LANES], 0.0)
                    vals_out[u * dpt + j] = jnp.sum(picked, axis=0, keepdims=True)

        def drain(depth):
            while sum(kind == "sweep" for kind, *_ in pending) > depth:
                pop()
            if depth == 0:
                while pending:
                    pop()

        def finish(b):
            acc = sums.pop(b)
            acc = acc[0] + acc[1]
            acc = acc[:, :LANES] + acc[:, LANES:]
            at = block_of(b)
            mass_rows[b] = jnp.sum(acc, axis=0, keepdims=True)
            if b == 0:
                mass_in[me] = mass_rows[b]
                dests = own_half
            else:
                dests = [at * dph + j for j in around]
            for d in dests:
                pltpu.make_async_remote_copy(
                    src_ref=mass_rows.at[b], dst_ref=mass_in.at[me],
                    send_sem=mass_send, recv_sem=mass_recv,
                    device_id=(d), device_id_type=LOGICAL).start()

        def gather(u, k):
            j, r = k // capacity, k % capacity
            rows_v[u * dpt + j, pl.ds(r, 1), :] = corpus_f[pl.ds(ids_sm[u * dpt + j, 0, r], 1), :]

        def widen(k):
            size = rows_dev // (2 * PIECES)
            at = pl.ds(k * size, size)
            corpus_f[at, :] = corpus_v[at, :].astype(jnp.float32)

        def stage(b, m, pair):
            if pair is not None:
                at = pair[0] * dpt + 2 * pair[1]
                push(m, diagonal(rows_v[at].astype(jnp.bfloat16), rows_v[at + 1].astype(jnp.bfloat16)))
            push(m, weights(b))

        def reply(m, u, a):
            first = askers[u] * dpt + 2 * a
            q = q_full[pl.ds(pl.multiple_of(first * owned, 2 * owned), 2 * owned), :]
            pltpu.matmul_acc_lhs(
                extra[m], jnp.concatenate([q[:owned], q[owned:]], axis=1), load_staged_rhs=staged[m].pop(0))
            pending.append(("pair", m, extra[m], (u, a)))

        acts = dict(
            reach=reach_up, hand=hand_over, ids=stage_ids, sm=lambda u: to_smem(u).wait(), vals=send_vals,
            mass=finish, arrive=arrive)
        total = 2 * tiles * PIECES
        answers = {h + m: (u, 2 * k + m) for u in UNITS for k, h in enumerate(UNITS[u][2]) for m in range(2)}
        for step in range(total):
            b, piece, m = step // PIECES, step % PIECES, step % 2
            if step == 0:
                mark("arrive0")
                reach_up(1)
                arrive(0)
                load.wait()
                for side in range(2):
                    push(side, weights(0))
            for name, arg in PLAN.get(step, ()):
                mark(f"{name}{arg}")
                acts[name](arg)
            if step in PLAN or step == 0:
                mark(f"go{step}")
            if step in FENCES:
                pl.semaphore_signal(fence_sem, inc=1)
            if piece == 0:
                at = pl.ds(pl.multiple_of(block_of(b) * LANES, LANES), LANES)
                cut = thr_ref[:, at].astype(jnp.float32) * 0.01
                cut = jnp.concatenate([cut, cut], axis=1)
            if step in answers:
                reply(m, *answers[step])
            at = pl.ds(piece * ROWS, ROWS)
            lhs = jnp.concatenate(
                [corpus_v[at, :], corpus_v[pl.ds(rows_dev // 2 + piece * ROWS, ROWS), :]], axis=1)
            ref = ranges[m][count[m] % RANGES]
            count[m] += 1
            pltpu.matmul_acc_lhs(ref, lhs, load_staged_rhs=staged[m].pop(0) if staged[m] and step % 16 < 2 else None)
            pending.append(("sweep", m, ref, (b, cut)))
            for u, (s0, length, _) in UNITS.items():
                if s0 <= step < s0 + length:
                    for k in range((step - s0) * dpt * capacity // length, (step - s0 + 1) * dpt * capacity // length):
                        gather(u, k)
            if step < 2 * PIECES:
                widen(step)
            ahead = step + AHEAD
            if ahead % 16 < 2 and 16 <= ahead < total and (ahead % PIECES < 2 or ahead in answers):
                stage(ahead // PIECES, ahead % 2, answers.get(ahead))
            drain(2 * LAG)
        drain(0)
        finish(2 * tiles - 1)

    pl.run_scoped(
        stream,
        *[pltpu.ACC(0)((ROWS, TILE), jnp.float32)] * RANGES,
        *[pltpu.ACC(1)((ROWS, TILE), jnp.float32)] * RANGES,
        pltpu.ACC(0)((owned, TILE), jnp.float32),
        pltpu.ACC(1)((owned, TILE), jnp.float32))

    mark("valswait")
    bulk_wait(vals_in.at[pl.ds(0, n - 1)], vals_recv)
    mark("spread")
    values = jnp.concatenate([vals_in[t] for t in range(n)], axis=0)
    top = values.astype(jnp.bfloat16)
    rest = values - top.astype(jnp.float32)
    mid = rest.astype(jnp.bfloat16)
    last = (rest - mid.astype(jnp.float32)).astype(jnp.bfloat16)
    upper_part = jnp.concatenate([top, mid], axis=1)
    lower_part = jnp.concatenate([last, jnp.zeros_like(last)], axis=1)
    cand = cand_pad[...]
    target = lax.shift_right_arithmetic(cand, jnp.int32(id_bits))
    dest = lax.broadcasted_iota(jnp.int32, (n, LANES), 0)

    def spread(*refs):
        for i in range(owned // 2):
            place = places[:, 2 * i * LANES:2 * (i + 1) * LANES]
            pltpu.matmul_push_rhs(
                jnp.concatenate([place, place], axis=0), staging_register=i // 2 % 2, mxu_index=i % 2)
            pltpu.matmul_acc_lhs(refs[i % 2][i // 2], upper_part, load_staged_rhs=i // 2 % 2)
            pltpu.matmul_acc_lhs(refs[i % 2][i // 2], lower_part)
        for i in range(owned // 2):
            both = pltpu.matmul_pop(refs[i % 2][i // 2])
            for e in range(2):
                q = 2 * i + e
                ans_out[q:q + 1, :] = jnp.sum(
                    jnp.where(target[q:q + 1] == dest, both[:, e * LANES:(e + 1) * LANES], 0.0),
                    axis=0, keepdims=True)[:, :per_query]

    pl.run_scoped(
        spread,
        (pltpu.ACC(0)((n, TILE), jnp.float32),) * (owned // 4),
        (pltpu.ACC(1)((n, TILE), jnp.float32),) * (owned // 4))

    mark("masswait")
    bulk_wait(mass_in.at[pl.ds(0, n - 1)], mass_recv)
    mark("masssum")
    mass = mass_in[0]
    for t in range(1, n):
        mass = mass + mass_in[t]
    mass = mass * (8.0 / npass_all)
    per_row = LANES // owned
    result = mass
    for u in range(1, per_row):
        result = jnp.where(me % per_row == u, pltpu.roll(mass, LANES - u * owned, 1), result)
    mass_out[...] = result[:, :owned]

    mark("sendwaits")
    pl.semaphore_wait(fence_sem, len(FENCES))
    bulk_wait(q_in.at[pl.ds(0, dpt - 1 + (tiles - 1) * dpc)], q_send)
    bulk_wait(q_in.at[pl.ds(0, (tiles - 1) * dpc)], hand_send)
    bulk_wait(ids_in.at[pl.ds(0, n - 1)], ids_send)
    bulk_wait(vals_in.at[pl.ds(0, n - 1)], vals_send)
    bulk_wait(mass_in.at[pl.ds(0, n - 1)], mass_send)
    mark(None)


def fused_body(n, nf, queries, corpus, candidates, threshold):
    rows_dev, width = corpus.shape
    owned, per_query = candidates.shape
    nq = n * owned
    tiles = nq // TILE
    capacity = (owned * per_query + n - 1) // n
    mass, answers = pl.pallas_call(
        functools.partial(kernel, n, nf, rows_dev * n, capacity),
        out_shape=(
            pltpu.VMEM((1, owned), jnp.float32),
            pltpu.VMEM((owned, per_query), jnp.float32),
        ),
        in_specs=[pl.BlockSpec(memory_space=pl.ANY)] * 4,
        out_specs=[pl.BlockSpec(memory_space=pltpu.VMEM)] * 2,
        scratch_shapes=[
            pltpu.VMEM(queries.shape, jnp.bfloat16),
            pltpu.VMEM((1, nq), jnp.int32),
            pltpu.VMEM((owned, per_query), jnp.int32),
            pltpu.VMEM((rows_dev, width), jnp.bfloat16),
            pltpu.VMEM((rows_dev, width), jnp.float32),
            pltpu.VMEM((owned, LANES), jnp.bfloat16),
            pltpu.VMEM((n, owned, LANES), jnp.bfloat16),
            pltpu.VMEM((nq, LANES), jnp.bfloat16),
            pltpu.VMEM((owned, LANES), jnp.int32),
            pltpu.VMEM((LANES, owned * LANES), jnp.bfloat16),
            pltpu.VMEM((n, 1, LANES), jnp.int32),
            pltpu.VMEM((n, 1, LANES), jnp.int32),
            pltpu.VMEM((n, 1, LANES), jnp.int32),
            pltpu.SMEM((n, 1, LANES), jnp.int32),
            pltpu.VMEM((n, LANES, LANES), jnp.float32),
            pltpu.VMEM((n, 1, LANES), jnp.float32),
            pltpu.VMEM((n, 1, LANES), jnp.float32),
            pltpu.VMEM((nq // LANES, 1, LANES), jnp.float32),
            pltpu.VMEM((n, 1, LANES), jnp.float32),
            pltpu.SemaphoreType.DMA((3,)),
            pltpu.SemaphoreType.DMA,
            pltpu.SemaphoreType.DMA((tiles,)),
            pltpu.SemaphoreType.REGULAR((tiles,)),
            pltpu.SemaphoreType.REGULAR,
            pltpu.SemaphoreType.DMA,
            pltpu.SemaphoreType.DMA((tiles + 2,)),
            pltpu.SemaphoreType.DMA,
            pltpu.SemaphoreType.DMA((tiles,)),
            pltpu.SemaphoreType.DMA,
            pltpu.SemaphoreType.DMA((tiles,)),
            pltpu.SemaphoreType.DMA,
            pltpu.SemaphoreType.DMA,
            pltpu.SemaphoreType.DMA,
            pltpu.SemaphoreType.DMA,
        ],
        compiler_params=pltpu.CompilerParams(
            collective_id=0, has_side_effects=True),
    )(queries, threshold.reshape(1, nq), candidates, corpus)
    return mass.reshape(owned), answers


def plain_body(queries, corpus, candidates, threshold):
    rows_dev = corpus.shape[0]
    width = corpus.shape[1]
    shards = lax.axis_size("rows") * lax.axis_size("feat")
    owned_queries = candidates.shape[0]
    per_query = candidates.shape[1]
    npass_all = rows_dev * shards
    cutoff = threshold.astype(jnp.float32) * 0.01
    owner = lax.axis_index(("rows", "feat"))
    full_rows = lax.all_gather(queries, "feat", axis=1, tiled=True)
    whole = lax.all_gather(full_rows, "rows", axis=0, tiled=True)
    query_count = whole.shape[0]
    block = 2048
    corpus_blocks = corpus.reshape(rows_dev // block, block, width)

    def visit(total, block_rows):
        scores = lax.dot_general(
            whole, block_rows, (((1,), (1,)), ((), ())), preferred_element_type=jnp.float32
        )
        return (total + jnp.sum(jnp.maximum(scores - cutoff[:, None], 0.0), axis=1), None)

    total, _ = lax.scan(visit, jnp.zeros((query_count,), jnp.float32), corpus_blocks)
    flat_ids = candidates.reshape(-1)
    total_ids = flat_ids.shape[0]
    capacity = (total_ids + shards - 1) // shards
    target = flat_ids // rows_dev
    onehot = (target[:, None] == jnp.arange(shards, dtype=jnp.int32)[None, :]).astype(jnp.int32)
    before = jnp.cumsum(onehot, axis=0) - onehot
    rank = jnp.sum(before * onehot, axis=1)
    query_ids = owner * owned_queries + jnp.arange(total_ids, dtype=jnp.int32) // per_query
    fields = jnp.stack([flat_ids - target * rows_dev, query_ids], axis=1)
    send_both = jnp.zeros((shards, capacity, 2), jnp.int32).at[target, rank].set(fields)
    n_rows = lax.axis_size("rows")
    n_feat = lax.axis_size("feat")
    received = lax.all_to_all(
        lax.all_to_all(
            send_both.reshape(n_rows, n_feat, capacity * 2),
            "rows",
            split_axis=0,
            concat_axis=0,
            tiled=True,
        ),
        "feat",
        split_axis=1,
        concat_axis=1,
        tiled=True,
    )
    received = received.reshape(shards * capacity, 2)
    picked = corpus[received[:, 0]]
    asked = whole[received[:, 1]]
    values = jnp.einsum("kd,kd->k", picked, asked, preferred_element_type=jnp.float32).reshape(
        n_rows, n_feat, capacity
    )
    partials = total.reshape(n_rows, n_feat, owned_queries)
    answers, mass_parts = (
        lax.all_to_all(
            lax.all_to_all(values, "rows", split_axis=0, concat_axis=0, tiled=True),
            "feat",
            split_axis=1,
            concat_axis=1,
            tiled=True,
        ),
        lax.all_to_all(
            lax.all_to_all(partials, "rows", split_axis=0, concat_axis=0, tiled=True),
            "feat",
            split_axis=1,
            concat_axis=1,
            tiled=True,
        ),
    )
    exceed = jnp.sum(mass_parts, axis=(0, 1)) * (8.0 / npass_all)
    candidate_scores = answers.reshape(shards, capacity)[target, rank].reshape(
        owned_queries, per_query
    )
    return (exceed, candidate_scores)


def body(queries, corpus, candidates, threshold):
    nf = lax.axis_size("feat")
    n = lax.axis_size("rows") * nf
    rows_dev, width = corpus.shape
    owned, per_query = candidates.shape
    capacity = (owned * per_query + n - 1) // n
    fits = (
        nf == 2
        and width == LANES
        and queries.shape == (2 * owned, LANES // 2)
        and owned % 32 == 0
        and LANES % owned == 0
        and per_query <= LANES
        and capacity <= LANES
        and n % 8 == 0
        and (n * owned) % TILE == 0
        and n * owned == 4 * TILE
        and rows_dev == 2 * ROWS * PIECES
        and rows_dev & (rows_dev - 1) == 0
    )
    if fits:
        return fused_body(n, nf, queries, corpus, candidates, threshold)
    return plain_body(queries, corpus, candidates, threshold)


def solution(mesh):
    return jax.shard_map(
        body,
        mesh=mesh,
        in_specs=(P("rows", "feat"), P(("rows", "feat"), None), P(("rows", "feat"), None), P()),
        out_specs=(P(("rows", "feat")), P(("rows", "feat"), None)),
        check_vma=False,
    )
```

```python
import functools

import jax
import jax.numpy as jnp
from jax import lax
from jax.experimental import pallas as pl
from jax.experimental.pallas import tpu as pltpu
from jax.sharding import PartitionSpec as P

LANES = 128
TILE = 256
ROWS = 256
PIECES = 32
WIDEN = 512
RANGES = 3
LAG = 2
AHEAD = 5
UNITS = {
    0: (74, 32, (96, 112)), 1: (106, 22, (128, 144)), 2: (154, 32, (176, 192)),
}
PLAN = {
    20: (("arrive", 1),),
    38: (("mass", 0), ("reach", 2), ("hand", 1), ("reach", 3)),
    54: (("ids", 0),),
    58: (("arrive", 2),),
    70: (("mass", 1), ("sm", 0)),
    96: (("ids", 1), ("hand", 2)),
    106: (("mass", 2), ("sm", 1)),
    118: (("vals", 0),),
    122: (("arrive", 4),),
    134: (("mass", 3), ("ids", 2)),
    150: (("vals", 1), ("hand", 3), ("sm", 2)),
    166: (("mass", 4), ("ids", 3)),
    172: (("arrive", 6),),
    198: (("mass", 5), ("vals", 2)),
    230: (("mass", 6), ("sm", 3)),
}
FENCES = frozenset(range(0, 192, 8))
LOGICAL = pl.DeviceIdType.LOGICAL


def mark(name):
    pass


def bulk_wait(ref, sem):
    pltpu.make_async_copy(ref, ref, sem).wait()


def kernel(
    n, nf, npass_all, capacity,
    q_hbm, thr_hbm, cand_hbm, corpus_ref,
    mass_out, ans_out,
    q_ref, thr_ref, cand_ref, corpus_v, corpus_f, q_pack, q_in, q_full, cand_pad, places,
    ids_out, ids_in, ids_at, ids_sm, rows_v, vals_out, vals_in, mass_rows, mass_in,
    small_sem, load_sem, sm_sem, in_sem, fence_sem, q_send, q_recv, hand_send, hand_recv,
    ids_send, ids_recv, vals_send, vals_recv, mass_send, mass_recv,
):
    rows_dev, width = corpus_v.shape
    owned, per_query = cand_ref.shape
    nq = q_full.shape[0]
    half = q_ref.shape[1]
    tiles = nq // TILE
    dpt = TILE // owned
    dph = dpt // 2
    chips = n // nf
    dpc = dpt // nf
    core = lax.axis_index("feat")
    me = lax.axis_index("rows") * nf + core
    my_tile = me // dpt
    my_j = me % dpt
    my_half = my_j // dph
    my_h = my_j % dph
    id_bits = rows_dev.bit_length() - 1

    def table(values):
        out = values[0]
        for k in range(1, tiles):
            out = out + (values[k] - values[k - 1]) * ((my_tile + tiles - 1 - k) // (tiles - 1))
        return out

    planes = [my_tile, table((1, 0, 1, 2)), table((2, 2, 0, 0)), table((3, 3, 3, 1))]
    askers = [table(row) for row in ((0, 0, 1, 2), (1, 1, 0, 0), (2, 2, 2, 1), (3, 3, 3, 3))]

    load = pltpu.make_async_copy(corpus_ref, corpus_v, load_sem)
    small = [
        pltpu.make_async_copy(src, dst, small_sem.at[k])
        for k, (src, dst) in enumerate(((q_hbm, q_ref), (cand_hbm, cand_ref), (thr_hbm, thr_ref)))]
    for copy in small:
        copy.start()
    load.start()

    around = [(my_h + i) % dph for i in range(dph)]
    own_half = [my_tile * dpt + my_half * dph + j for j in around[1:]]
    other_half = [my_tile * dpt + (1 - my_half) * dph + j for j in around]
    neighbours = own_half + other_half

    def plane_of(t):
        return [t * dpt + (my_j + j) % dpt for j in range(dpt)]

    def same_core_of(t):
        return [(t * dpc + (my_j // nf + j) % dpc) * nf + core for j in range(dpc)]

    barrier = pltpu.get_barrier_semaphore()

    def signal(sem, d):
        pl.semaphore_signal(sem, inc=1, device_id=(d), device_id_type=LOGICAL)

    mark("start")
    for d in neighbours:
        signal(barrier, d)
    for k in range(1, tiles):
        @pl.when(my_tile + k < tiles)
        def _():
            for d in plane_of(my_tile + k):
                signal(barrier, d)

    mark("smallwait")
    for copy in small:
        copy.wait()
    mark("pack")
    q_local = q_ref[...].astype(jnp.float32)
    mine = jnp.concatenate([q_local[:owned], q_local[owned:]], axis=1).astype(jnp.bfloat16)
    q_pack[...] = mine
    my_place = core * chips + me // nf
    q_in[my_place] = mine

    mark("barrier")
    pl.semaphore_wait(barrier, dpt - 1 + my_tile * dpt)
    mark("sends1")

    def send_queries(d, sem):
        pltpu.make_async_remote_copy(
            src_ref=q_pack, dst_ref=q_in.at[my_place], send_sem=q_send, recv_sem=sem,
            device_id=(d), device_id_type=LOGICAL).start()

    def send_ids(d):
        pltpu.make_async_remote_copy(
            src_ref=ids_out.at[d], dst_ref=ids_in.at[me], send_sem=ids_send, recv_sem=ids_recv.at[my_tile],
            device_id=(d), device_id_type=LOGICAL).start()

    for d in own_half:
        send_queries(d, q_recv.at[tiles])
    for d in other_half:
        send_queries(d, q_recv.at[tiles + 1])
    for k in range(1, tiles):
        @pl.when(my_tile >= k)
        def _():
            signal(in_sem.at[my_tile], me - k * dpt)
            for d in same_core_of(my_tile - k):
                send_queries(d, q_recv.at[my_tile])

    mark("sort")
    cand_pad[...] = jnp.full(cand_pad.shape, -1, jnp.int32)
    cand_pad[:, :per_query] = cand_ref[...]
    cand = cand_pad[...]
    target = lax.shift_right_arithmetic(cand, jnp.int32(id_bits))
    local = jnp.bitwise_and(cand, jnp.int32(rows_dev - 1))
    low = jnp.bitwise_and(local, jnp.int32(LANES - 1)).astype(jnp.float32)
    high = lax.shift_right_arithmetic(local, jnp.int32(7)).astype(jnp.float32)
    dest = lax.broadcasted_iota(jnp.int32, (n, LANES), 0)
    hot = [jnp.where(target[q:q + 1] == dest, 1.0, 0.0) for q in range(owned)]
    row_i = lax.broadcasted_iota(jnp.int32, (LANES, 2 * LANES), 0)
    col_i = lax.broadcasted_iota(jnp.int32, (LANES, 2 * LANES), 1)
    upper = jnp.where((row_i < col_i) | (col_i >= LANES), 1.0, 0.0).astype(jnp.bfloat16)

    def sort(count0, count1, field0, field1):
        blank = jnp.zeros((TILE, LANES), jnp.bfloat16)
        chunk = TILE // n
        refs = (count0, count1)
        for m in range(2):
            pltpu.matmul_push_rhs(
                jnp.concatenate([upper, jnp.zeros_like(upper)], axis=0), staging_register=0, mxu_index=m)
        for i in range(owned // chunk):
            part = jnp.concatenate(hot[i * chunk:(i + 1) * chunk], axis=0).astype(jnp.bfloat16)
            pltpu.matmul_acc_lhs(
                refs[i % 2][i // 2], jnp.concatenate([part, blank], axis=1),
                load_staged_rhs=0 if i < 2 else None)
        base = jnp.zeros((n, LANES), jnp.float32)
        slot = lax.broadcasted_iota(jnp.int32, (LANES, LANES), 0).astype(jnp.float32)
        fields = []
        for q in range(owned):
            if q % chunk == 0:
                counts = pltpu.matmul_pop(refs[q // chunk % 2][q // chunk // 2])
            block = counts[q % chunk * n:(q % chunk + 1) * n]
            rank = jnp.sum(hot[q] * (block[:, :LANES] + base), axis=0, keepdims=True)
            base = base + block[:, LANES:]
            places[:, q * LANES:(q + 1) * LANES] = jnp.where(rank == slot, 1.0, 0.0).astype(jnp.bfloat16)
            fields.append(jnp.concatenate(
                [hot[q] * low[q:q + 1], hot[q] * high[q:q + 1], hot[q] * float(q)], axis=0
            ).astype(jnp.bfloat16))
        sums = (field0, field1)
        turns = owned // 4
        for i in range(turns):
            pairs = (2 * i, owned // 2 + 2 * i)
            pltpu.matmul_push_rhs(
                jnp.concatenate([places[:, q * LANES:(q + 2) * LANES] for q in pairs], axis=0),
                staging_register=i // 2 % 2, mxu_index=i % 2, transpose=True)
            pltpu.matmul_acc_lhs(
                sums[i % 2],
                jnp.concatenate([jnp.concatenate(fields[q:q + 2], axis=1) for q in pairs], axis=0),
                load_staged_rhs=i // 2 % 2)
        total = pltpu.matmul_pop(field0) + pltpu.matmul_pop(field1)
        sorted_fields = total[:3 * n, :LANES] + total[3 * n:, LANES:]
        packed = (
            sorted_fields[:n] + sorted_fields[n:2 * n] * float(LANES) + sorted_fields[2 * n:] * float(rows_dev)
        ).astype(jnp.int32)
        for t in range(n):
            ids_out[t] = packed[t:t + 1]
        ids_in[me] = ids_out[me]

    pl.run_scoped(
        sort,
        (pltpu.ACC(0)((TILE, TILE), jnp.float32),) * (owned * n // TILE // 2),
        (pltpu.ACC(1)((TILE, TILE), jnp.float32),) * (owned * n // TILE // 2),
        pltpu.ACC(0)((6 * n, TILE), jnp.float32),
        pltpu.ACC(1)((6 * n, TILE), jnp.float32))

    mark("sends2")
    for d in neighbours:
        send_ids(d)
    for k in range(1, tiles):
        @pl.when(my_tile >= k)
        def _():
            for d in plane_of(my_tile - k):
                send_ids(d)

    def reach_up(k):
        @pl.when(my_tile + k < tiles)
        def _():
            pl.semaphore_wait(in_sem.at[my_tile + k], 1)
            for d in plane_of(my_tile + k):
                send_ids(d)
            for d in same_core_of(my_tile + k):
                send_queries(d, q_recv.at[my_tile])

    def hand_over(p):
        blocks_of = q_in.at[pl.ds(core * chips + planes[p] * dpc, dpc)]
        bulk_wait(blocks_of, q_recv.at[planes[p]])
        pltpu.make_async_remote_copy(
            src_ref=blocks_of, dst_ref=blocks_of, send_sem=hand_send, recv_sem=hand_recv.at[planes[p]],
            device_id=(me + 1 - 2 * core), device_id_type=LOGICAL).start()

    left = lax.broadcasted_iota(jnp.int32, (owned, LANES), 1) < half

    def unpack(chip):
        f0 = q_in[chip].astype(jnp.float32)
        f1 = q_in[chips + chip].astype(jnp.float32)
        both = jnp.concatenate(
            [jnp.where(left, f0, pltpu.roll(f1, half, 1)), jnp.where(left, pltpu.roll(f0, half, 1), f1)], axis=0)
        q_full[pl.ds(pl.multiple_of(chip * 2 * owned, 2 * owned), 2 * owned), :] = both.astype(jnp.bfloat16)

    order = [(b // 2, b % 2) for b in range(2 * tiles)]

    def arrive(b):
        p, side = order[b]
        if b == 0:
            bulk_wait(q_in.at[pl.ds(0, dph - 1)], q_recv.at[tiles])
            first, many = my_tile * dpc + my_half * (dpc // 2), dpc // 2
        elif b == 1:
            bulk_wait(q_in.at[pl.ds(0, dph)], q_recv.at[tiles + 1])
            first, many = my_tile * dpc + (1 - my_half) * (dpc // 2), dpc // 2
        elif side == 0:
            bulk_wait(q_in.at[pl.ds(0, dpc)], hand_recv.at[planes[p]])
            first, many = planes[p] * dpc, dpc
        else:
            many = 0
        for g in range(many):
            unpack(first + g)

    def block_of(b):
        p, side = order[b]
        if b == 0:
            return my_tile * 2 + my_half
        if b == 1:
            return my_tile * 2 + 1 - my_half
        return planes[p] * 2 + side

    def stage_ids(u):
        @pl.when(my_tile == u)
        def _():
            bulk_wait(ids_in.at[pl.ds(0, dpt - 1)], ids_recv.at[askers[u]])

        @pl.when(my_tile != u)
        def _():
            bulk_wait(ids_in.at[pl.ds(0, dpt)], ids_recv.at[askers[u]])
        ids_at[pl.ds(u * dpt, dpt)] = jnp.bitwise_and(
            ids_in[pl.ds(pl.multiple_of(askers[u] * dpt, dpt), dpt)], jnp.int32(rows_dev - 1))
        to_smem(u).start()

    def to_smem(u):
        at = pl.ds(u * dpt, dpt)
        return pltpu.make_async_copy(ids_at.at[at], ids_sm.at[at], sm_sem.at[u])

    def send_vals(u):
        def send(at):
            pltpu.make_async_remote_copy(
                src_ref=vals_out.at[u * dpt + at], dst_ref=vals_in.at[me], send_sem=vals_send, recv_sem=vals_recv,
                device_id=(askers[u] * dpt + at), device_id_type=LOGICAL).start()

        for j in range(1, dpt):
            send((my_j + j) % dpt)

        @pl.when(my_tile != u)
        def _():
            send(my_j)

        @pl.when(my_tile == u)
        def _():
            vals_in[me] = vals_out[u * dpt + my_j]

    who_q = lax.broadcasted_iota(jnp.int32, (owned, LANES), 0)
    in_use = lax.broadcasted_iota(jnp.int32, (owned, LANES), 1) < capacity
    zeros = jnp.zeros((LANES, LANES), jnp.bfloat16)

    def diagonal(a, b):
        z = zeros[:a.shape[0]]
        return jnp.concatenate([jnp.concatenate([a, z], axis=1), jnp.concatenate([z, b], axis=1)], axis=0)

    def stream(*accs):
        ranges = (accs[:RANGES], accs[RANGES:2 * RANGES])
        extra = accs[2 * RANGES:]
        turn = [0, 0]
        staged = [[], []]
        pending = []
        sums = {}
        count = [0, 0]

        def push(m, value):
            r = turn[m]
            turn[m] = 1 - r
            pltpu.matmul_push_rhs(value, staging_register=r, mxu_index=m, transpose=True)
            staged[m].append(r)
            assert len(staged[m]) <= 2

        def weights(b):
            at = block_of(b)
            q = q_full[pl.ds(pl.multiple_of(at * LANES, LANES), LANES), :]
            return diagonal(q, q)

        def pop():
            kind, m, ref, data = pending.pop(0)
            got = pltpu.matmul_pop(ref)
            if kind == "sweep":
                over = jnp.maximum(got - data[1], 0.0).reshape(ROWS // 16, 2, 8, 2 * LANES)
                part = jnp.sum(over, axis=0)
                sums[data[0]] = sums[data[0]] + part if data[0] in sums else part
            else:
                u, a = data
                for e in range(2):
                    j = 2 * a + e
                    who = lax.shift_right_arithmetic(
                        ids_in[askers[u] * dpt + j], jnp.int32(id_bits))
                    picked = jnp.where((who == who_q) & in_use, got[:, e * LANES:(e + 1) * LANES], 0.0)
                    vals_out[u * dpt + j] = jnp.sum(picked, axis=0, keepdims=True)

        def drain(depth):
            while sum(kind == "sweep" for kind, *_ in pending) > depth:
                pop()
            if depth == 0:
                while pending:
                    pop()

        def finish(b):
            acc = sums.pop(b)
            acc = acc[0] + acc[1]
            acc = acc[:, :LANES] + acc[:, LANES:]
            at = block_of(b)
            mass_rows[b] = jnp.sum(acc, axis=0, keepdims=True)
            if b == 0:
                mass_in[me] = mass_rows[b]
                dests = own_half
            else:
                dests = [at * dph + j for j in around]
            for d in dests:
                pltpu.make_async_remote_copy(
                    src_ref=mass_rows.at[b], dst_ref=mass_in.at[me],
                    send_sem=mass_send, recv_sem=mass_recv,
                    device_id=(d), device_id_type=LOGICAL).start()

        def gather(u, k):
            j, r = k // capacity, k % capacity
            rows_v[u * dpt + j, pl.ds(r, 1), :] = corpus_f[pl.ds(ids_sm[u * dpt + j, 0, r], 1), :]

        def stage(b, m, pair):
            if pair is not None:
                at = pair[0] * dpt + 2 * pair[1]
                push(m, diagonal(rows_v[at].astype(jnp.bfloat16), rows_v[at + 1].astype(jnp.bfloat16)))
            push(m, weights(b))

        def reply(m, u, a, spare=0):
            ref = extra[m + 2 * spare]
            first = askers[u] * dpt + 2 * a
            q = q_full[pl.ds(pl.multiple_of(first * owned, 2 * owned), 2 * owned), :]
            pltpu.matmul_acc_lhs(
                ref, jnp.concatenate([q[:owned], q[owned:]], axis=1), load_staged_rhs=staged[m].pop(0))
            pending.append(("pair", m, ref, (u, a)))

        acts = dict(
            reach=reach_up, hand=hand_over, ids=stage_ids, sm=lambda u: to_smem(u).wait(), vals=send_vals,
            mass=finish, arrive=arrive)
        total = 2 * tiles * PIECES
        answers = {h + m: (u, 2 * k + m) for u in UNITS for k, h in enumerate(UNITS[u][2]) for m in range(2)}
        for step in range(total):
            b, piece, m = step // PIECES, step % PIECES, step % 2
            if step == 0:
                mark("arrive0")
                arrive(0)
                for side in range(2):
                    push(side, weights(0))
            for name, arg in PLAN.get(step, ()):
                mark(f"{name}{arg}")
                acts[name](arg)
            if step in PLAN or step == 0:
                mark(f"go{step}")
            if step in FENCES:
                pl.semaphore_signal(fence_sem, inc=1)
            if piece == 0:
                at = pl.ds(pl.multiple_of(block_of(b) * LANES, LANES), LANES)
                cut = thr_ref[:, at].astype(jnp.float32) * 0.01
                cut = jnp.concatenate([cut, cut], axis=1)
            if step in answers:
                reply(m, *answers[step])
            at = pl.ds(piece * ROWS, ROWS)
            lhs = jnp.concatenate(
                [corpus_v[at, :], corpus_v[pl.ds(rows_dev // 2 + piece * ROWS, ROWS), :]], axis=1)
            ref = ranges[m][count[m] % RANGES]
            count[m] += 1
            pltpu.matmul_acc_lhs(ref, lhs, load_staged_rhs=staged[m].pop(0) if staged[m] and step % 16 < 2 else None)
            pending.append(("sweep", m, ref, (b, cut)))
            for u, (s0, length, _) in UNITS.items():
                if s0 <= step < s0 + length:
                    for k in range((step - s0) * dpt * capacity // length, (step - s0 + 1) * dpt * capacity // length):
                        gather(u, k)
            ahead = step + AHEAD
            if ahead % 16 < 2 and 16 <= ahead < total and (ahead % PIECES < 2 or ahead in answers):
                stage(ahead // PIECES, ahead % 2, answers.get(ahead))
            drain(2 * LAG)
        drain(0)
        finish(2 * tiles - 1)

        mark("last")
        u = tiles - 1
        for k in range(dpt * capacity):
            gather(u, k)
        for a in range(dpt // 2):
            at = u * dpt + 2 * a
            push(a % 2, diagonal(rows_v[at].astype(jnp.bfloat16), rows_v[at + 1].astype(jnp.bfloat16)))
            reply(a % 2, u, a, a // 2)
        drain(0)
        send_vals(u)

    mark("reach1")
    reach_up(1)
    load.wait()
    mark("widen")

    def widen(b, carry):
        at = pl.ds(pl.multiple_of(b * WIDEN, WIDEN), WIDEN)
        corpus_f[at, :] = corpus_v[at, :].astype(jnp.float32)
        return carry
    lax.fori_loop(0, rows_dev // WIDEN, widen, 0)

    pl.run_scoped(
        stream,
        *[pltpu.ACC(0)((ROWS, TILE), jnp.float32)] * RANGES,
        *[pltpu.ACC(1)((ROWS, TILE), jnp.float32)] * RANGES,
        *[pltpu.ACC(m % 2)((owned, TILE), jnp.float32) for m in range(4)])

    mark("valswait")
    bulk_wait(vals_in.at[pl.ds(0, n - 1)], vals_recv)
    mark("spread")
    values = jnp.concatenate([vals_in[t] for t in range(n)], axis=0)
    top = values.astype(jnp.bfloat16)
    rest = values - top.astype(jnp.float32)
    mid = rest.astype(jnp.bfloat16)
    last = (rest - mid.astype(jnp.float32)).astype(jnp.bfloat16)
    upper_part = jnp.concatenate([top, mid], axis=1)
    lower_part = jnp.concatenate([last, jnp.zeros_like(last)], axis=1)
    cand = cand_pad[...]
    target = lax.shift_right_arithmetic(cand, jnp.int32(id_bits))
    dest = lax.broadcasted_iota(jnp.int32, (n, LANES), 0)

    def spread(*refs):
        for i in range(owned // 2):
            place = places[:, 2 * i * LANES:2 * (i + 1) * LANES]
            pltpu.matmul_push_rhs(
                jnp.concatenate([place, place], axis=0), staging_register=i // 2 % 2, mxu_index=i % 2)
            pltpu.matmul_acc_lhs(refs[i % 2][i // 2], upper_part, load_staged_rhs=i // 2 % 2)
            pltpu.matmul_acc_lhs(refs[i % 2][i // 2], lower_part)
        for i in range(owned // 2):
            both = pltpu.matmul_pop(refs[i % 2][i // 2])
            for e in range(2):
                q = 2 * i + e
                ans_out[q:q + 1, :] = jnp.sum(
                    jnp.where(target[q:q + 1] == dest, both[:, e * LANES:(e + 1) * LANES], 0.0),
                    axis=0, keepdims=True)[:, :per_query]

    pl.run_scoped(
        spread,
        (pltpu.ACC(0)((n, TILE), jnp.float32),) * (owned // 4),
        (pltpu.ACC(1)((n, TILE), jnp.float32),) * (owned // 4))

    mark("masswait")
    bulk_wait(mass_in.at[pl.ds(0, n - 1)], mass_recv)
    mark("masssum")
    mass = mass_in[0]
    for t in range(1, n):
        mass = mass + mass_in[t]
    mass = mass * (8.0 / npass_all)
    per_row = LANES // owned
    result = mass
    for u in range(1, per_row):
        result = jnp.where(me % per_row == u, pltpu.roll(mass, LANES - u * owned, 1), result)
    mass_out[...] = result[:, :owned]

    mark("sendwaits")
    pl.semaphore_wait(fence_sem, len(FENCES))
    bulk_wait(q_in.at[pl.ds(0, dpt - 1 + (tiles - 1) * dpc)], q_send)
    bulk_wait(q_in.at[pl.ds(0, (tiles - 1) * dpc)], hand_send)
    bulk_wait(ids_in.at[pl.ds(0, n - 1)], ids_send)
    bulk_wait(vals_in.at[pl.ds(0, n - 1)], vals_send)
    bulk_wait(mass_in.at[pl.ds(0, n - 1)], mass_send)
    mark(None)


def fused_body(n, nf, queries, corpus, candidates, threshold):
    rows_dev, width = corpus.shape
    owned, per_query = candidates.shape
    nq = n * owned
    tiles = nq // TILE
    capacity = (owned * per_query + n - 1) // n
    mass, answers = pl.pallas_call(
        functools.partial(kernel, n, nf, rows_dev * n, capacity),
        out_shape=(
            pltpu.VMEM((1, owned), jnp.float32),
            pltpu.VMEM((owned, per_query), jnp.float32),
        ),
        in_specs=[pl.BlockSpec(memory_space=pl.ANY)] * 4,
        out_specs=[pl.BlockSpec(memory_space=pltpu.VMEM)] * 2,
        scratch_shapes=[
            pltpu.VMEM(queries.shape, jnp.bfloat16),
            pltpu.VMEM((1, nq), jnp.int32),
            pltpu.VMEM((owned, per_query), jnp.int32),
            pltpu.VMEM((rows_dev, width), jnp.bfloat16),
            pltpu.VMEM((rows_dev, width), jnp.float32),
            pltpu.VMEM((owned, LANES), jnp.bfloat16),
            pltpu.VMEM((n, owned, LANES), jnp.bfloat16),
            pltpu.VMEM((nq, LANES), jnp.bfloat16),
            pltpu.VMEM((owned, LANES), jnp.int32),
            pltpu.VMEM((LANES, owned * LANES), jnp.bfloat16),
            pltpu.VMEM((n, 1, LANES), jnp.int32),
            pltpu.VMEM((n, 1, LANES), jnp.int32),
            pltpu.VMEM((n, 1, LANES), jnp.int32),
            pltpu.SMEM((n, 1, LANES), jnp.int32),
            pltpu.VMEM((n, LANES, LANES), jnp.float32),
            pltpu.VMEM((n, 1, LANES), jnp.float32),
            pltpu.VMEM((n, 1, LANES), jnp.float32),
            pltpu.VMEM((nq // LANES, 1, LANES), jnp.float32),
            pltpu.VMEM((n, 1, LANES), jnp.float32),
            pltpu.SemaphoreType.DMA((3,)),
            pltpu.SemaphoreType.DMA,
            pltpu.SemaphoreType.DMA((tiles,)),
            pltpu.SemaphoreType.REGULAR((tiles,)),
            pltpu.SemaphoreType.REGULAR,
            pltpu.SemaphoreType.DMA,
            pltpu.SemaphoreType.DMA((tiles + 2,)),
            pltpu.SemaphoreType.DMA,
            pltpu.SemaphoreType.DMA((tiles,)),
            pltpu.SemaphoreType.DMA,
            pltpu.SemaphoreType.DMA((tiles,)),
            pltpu.SemaphoreType.DMA,
            pltpu.SemaphoreType.DMA,
            pltpu.SemaphoreType.DMA,
            pltpu.SemaphoreType.DMA,
        ],
        compiler_params=pltpu.CompilerParams(
            collective_id=0, has_side_effects=True),
    )(queries, threshold.reshape(1, nq), candidates, corpus)
    return mass.reshape(owned), answers


def plain_body(queries, corpus, candidates, threshold):
    rows_dev = corpus.shape[0]
    width = corpus.shape[1]
    shards = lax.axis_size("rows") * lax.axis_size("feat")
    owned_queries = candidates.shape[0]
    per_query = candidates.shape[1]
    npass_all = rows_dev * shards
    cutoff = threshold.astype(jnp.float32) * 0.01
    owner = lax.axis_index(("rows", "feat"))
    full_rows = lax.all_gather(queries, "feat", axis=1, tiled=True)
    whole = lax.all_gather(full_rows, "rows", axis=0, tiled=True)
    query_count = whole.shape[0]
    block = 2048
    corpus_blocks = corpus.reshape(rows_dev // block, block, width)

    def visit(total, block_rows):
        scores = lax.dot_general(
            whole, block_rows, (((1,), (1,)), ((), ())), preferred_element_type=jnp.float32
        )
        return (total + jnp.sum(jnp.maximum(scores - cutoff[:, None], 0.0), axis=1), None)

    total, _ = lax.scan(visit, jnp.zeros((query_count,), jnp.float32), corpus_blocks)
    flat_ids = candidates.reshape(-1)
    total_ids = flat_ids.shape[0]
    capacity = (total_ids + shards - 1) // shards
    target = flat_ids // rows_dev
    onehot = (target[:, None] == jnp.arange(shards, dtype=jnp.int32)[None, :]).astype(jnp.int32)
    before = jnp.cumsum(onehot, axis=0) - onehot
    rank = jnp.sum(before * onehot, axis=1)
    query_ids = owner * owned_queries + jnp.arange(total_ids, dtype=jnp.int32) // per_query
    fields = jnp.stack([flat_ids - target * rows_dev, query_ids], axis=1)
    send_both = jnp.zeros((shards, capacity, 2), jnp.int32).at[target, rank].set(fields)
    n_rows = lax.axis_size("rows")
    n_feat = lax.axis_size("feat")
    received = lax.all_to_all(
        lax.all_to_all(
            send_both.reshape(n_rows, n_feat, capacity * 2),
            "rows",
            split_axis=0,
            concat_axis=0,
            tiled=True,
        ),
        "feat",
        split_axis=1,
        concat_axis=1,
        tiled=True,
    )
    received = received.reshape(shards * capacity, 2)
    picked = corpus[received[:, 0]]
    asked = whole[received[:, 1]]
    values = jnp.einsum("kd,kd->k", picked, asked, preferred_element_type=jnp.float32).reshape(
        n_rows, n_feat, capacity
    )
    partials = total.reshape(n_rows, n_feat, owned_queries)
    answers, mass_parts = (
        lax.all_to_all(
            lax.all_to_all(values, "rows", split_axis=0, concat_axis=0, tiled=True),
            "feat",
            split_axis=1,
            concat_axis=1,
            tiled=True,
        ),
        lax.all_to_all(
            lax.all_to_all(partials, "rows", split_axis=0, concat_axis=0, tiled=True),
            "feat",
            split_axis=1,
            concat_axis=1,
            tiled=True,
        ),
    )
    exceed = jnp.sum(mass_parts, axis=(0, 1)) * (8.0 / npass_all)
    candidate_scores = answers.reshape(shards, capacity)[target, rank].reshape(
        owned_queries, per_query
    )
    return (exceed, candidate_scores)


def body(queries, corpus, candidates, threshold):
    nf = lax.axis_size("feat")
    n = lax.axis_size("rows") * nf
    rows_dev, width = corpus.shape
    owned, per_query = candidates.shape
    capacity = (owned * per_query + n - 1) // n
    fits = (
        nf == 2
        and width == LANES
        and queries.shape == (2 * owned, LANES // 2)
        and owned % 32 == 0
        and LANES % owned == 0
        and per_query <= LANES
        and capacity <= LANES
        and n % 8 == 0
        and (n * owned) % TILE == 0
        and n * owned == 4 * TILE
        and rows_dev == 2 * ROWS * PIECES
        and rows_dev & (rows_dev - 1) == 0
    )
    if fits:
        return fused_body(n, nf, queries, corpus, candidates, threshold)
    return plain_body(queries, corpus, candidates, threshold)


def solution(mesh):
    return jax.shard_map(
        body,
        mesh=mesh,
        in_specs=(P("rows", "feat"), P(("rows", "feat"), None), P(("rows", "feat"), None), P()),
        out_specs=(P(("rows", "feat")), P(("rows", "feat"), None)),
        check_vma=False,
    )
```

```python
import functools

import jax
import jax.numpy as jnp
from jax import lax
from jax.experimental import pallas as pl
from jax.experimental.pallas import tpu as pltpu
from jax.sharding import PartitionSpec as P

LANES = 128
TILE = 256
ROWS = 256
PIECES = 32
WIDEN = 512
RANGES = 3
LAG = 2
AHEAD = 5
UNITS = {
    0: (74, 32, (96, 112)), 1: (106, 22, (128, 144)), 2: (154, 32, (176, 192)),
}
PLAN = {
    20: (("arrive", 1), ("reach", 3)),
    38: (("mass", 0), ("reach", 2), ("hand", 1)),
    54: (("ids", 0),),
    58: (("arrive", 2),),
    70: (("mass", 1), ("sm", 0)),
    96: (("ids", 1), ("hand", 2)),
    106: (("mass", 2), ("sm", 1)),
    118: (("vals", 0),),
    122: (("arrive", 4),),
    134: (("mass", 3), ("ids", 2)),
    150: (("vals", 1), ("hand", 3), ("sm", 2)),
    166: (("mass", 4), ("ids", 3)),
    172: (("arrive", 6),),
    198: (("mass", 5), ("vals", 2)),
    230: (("mass", 6), ("sm", 3)),
}
FENCES = frozenset(range(0, 192, 8))
LOGICAL = pl.DeviceIdType.LOGICAL


def mark(name):
    pass


def bulk_wait(ref, sem):
    pltpu.make_async_copy(ref, ref, sem).wait()


def kernel(
    n, nf, npass_all, capacity,
    q_hbm, thr_hbm, cand_hbm, corpus_ref,
    mass_out, ans_out,
    q_ref, thr_ref, cand_ref, corpus_v, corpus_f, q_pack, q_in, q_full, cand_pad, places,
    ids_out, ids_in, ids_at, ids_sm, rows_v, vals_out, vals_in, mass_rows, mass_in,
    small_sem, load_sem, sm_sem, in_sem, fence_sem, q_send, q_recv, hand_send, hand_recv,
    ids_send, ids_recv, vals_send, vals_recv, mass_send, mass_recv,
):
    rows_dev, width = corpus_v.shape
    owned, per_query = cand_ref.shape
    nq = q_full.shape[0]
    half = q_ref.shape[1]
    tiles = nq // TILE
    dpt = TILE // owned
    dph = dpt // 2
    chips = n // nf
    dpc = dpt // nf
    core = lax.axis_index("feat")
    me = lax.axis_index("rows") * nf + core
    my_tile = me // dpt
    my_j = me % dpt
    my_half = my_j // dph
    my_h = my_j % dph
    id_bits = rows_dev.bit_length() - 1

    def table(values):
        out = values[0]
        for k in range(1, tiles):
            out = out + (values[k] - values[k - 1]) * ((my_tile + tiles - 1 - k) // (tiles - 1))
        return out

    planes = [my_tile, table((1, 0, 1, 2)), table((2, 2, 0, 0)), table((3, 3, 3, 1))]
    askers = [table(row) for row in ((0, 0, 1, 2), (1, 1, 0, 0), (2, 2, 2, 1), (3, 3, 3, 3))]

    load = pltpu.make_async_copy(corpus_ref, corpus_v, load_sem)
    small = [
        pltpu.make_async_copy(src, dst, small_sem.at[k])
        for k, (src, dst) in enumerate(((q_hbm, q_ref), (cand_hbm, cand_ref), (thr_hbm, thr_ref)))]
    for copy in small:
        copy.start()
    load.start()

    around = [(my_h + i) % dph for i in range(dph)]
    own_half = [my_tile * dpt + my_half * dph + j for j in around[1:]]
    other_half = [my_tile * dpt + (1 - my_half) * dph + j for j in around]
    neighbours = own_half + other_half

    def plane_of(t):
        return [t * dpt + (my_j + j) % dpt for j in range(dpt)]

    def same_core_of(t):
        return [(t * dpc + (my_j // nf + j) % dpc) * nf + core for j in range(dpc)]

    barrier = pltpu.get_barrier_semaphore()

    def signal(sem, d):
        pl.semaphore_signal(sem, inc=1, device_id=(d), device_id_type=LOGICAL)

    mark("start")
    for d in neighbours:
        signal(barrier, d)
    for k in range(1, tiles):
        @pl.when(my_tile + k < tiles)
        def _():
            for d in plane_of(my_tile + k):
                signal(barrier, d)

    mark("smallwait")
    for copy in small:
        copy.wait()
    mark("pack")
    q_local = q_ref[...].astype(jnp.float32)
    mine = jnp.concatenate([q_local[:owned], q_local[owned:]], axis=1).astype(jnp.bfloat16)
    q_pack[...] = mine
    my_place = core * chips + me // nf
    q_in[my_place] = mine

    mark("barrier")
    pl.semaphore_wait(barrier, dpt - 1 + my_tile * dpt)
    mark("sends1")

    def send_queries(d, sem):
        pltpu.make_async_remote_copy(
            src_ref=q_pack, dst_ref=q_in.at[my_place], send_sem=q_send, recv_sem=sem,
            device_id=(d), device_id_type=LOGICAL).start()

    def send_ids(d):
        pltpu.make_async_remote_copy(
            src_ref=ids_out.at[d], dst_ref=ids_in.at[me], send_sem=ids_send, recv_sem=ids_recv.at[my_tile],
            device_id=(d), device_id_type=LOGICAL).start()

    for d in own_half:
        send_queries(d, q_recv.at[tiles])
    for d in other_half:
        send_queries(d, q_recv.at[tiles + 1])
    for k in range(1, tiles):
        @pl.when(my_tile >= k)
        def _():
            signal(in_sem.at[my_tile], me - k * dpt)
            for d in same_core_of(my_tile - k):
                send_queries(d, q_recv.at[my_tile])

    mark("sort")
    cand_pad[...] = jnp.full(cand_pad.shape, -1, jnp.int32)
    cand_pad[:, :per_query] = cand_ref[...]
    cand = cand_pad[...]
    target = lax.shift_right_arithmetic(cand, jnp.int32(id_bits))
    local = jnp.bitwise_and(cand, jnp.int32(rows_dev - 1))
    low = jnp.bitwise_and(local, jnp.int32(LANES - 1)).astype(jnp.float32)
    high = lax.shift_right_arithmetic(local, jnp.int32(7)).astype(jnp.float32)
    dest = lax.broadcasted_iota(jnp.int32, (n, LANES), 0)
    hot = [jnp.where(target[q:q + 1] == dest, 1.0, 0.0) for q in range(owned)]
    row_i = lax.broadcasted_iota(jnp.int32, (LANES, 2 * LANES), 0)
    col_i = lax.broadcasted_iota(jnp.int32, (LANES, 2 * LANES), 1)
    upper = jnp.where((row_i < col_i) | (col_i >= LANES), 1.0, 0.0).astype(jnp.bfloat16)

    def sort(count0, count1, field0, field1):
        blank = jnp.zeros((TILE, LANES), jnp.bfloat16)
        chunk = TILE // n
        refs = (count0, count1)
        for m in range(2):
            pltpu.matmul_push_rhs(
                jnp.concatenate([upper, jnp.zeros_like(upper)], axis=0), staging_register=0, mxu_index=m)
        for i in range(owned // chunk):
            part = jnp.concatenate(hot[i * chunk:(i + 1) * chunk], axis=0).astype(jnp.bfloat16)
            pltpu.matmul_acc_lhs(
                refs[i % 2][i // 2], jnp.concatenate([part, blank], axis=1),
                load_staged_rhs=0 if i < 2 else None)
        base = jnp.zeros((n, LANES), jnp.float32)
        slot = lax.broadcasted_iota(jnp.int32, (LANES, LANES), 0).astype(jnp.float32)
        fields = []
        for q in range(owned):
            if q % chunk == 0:
                counts = pltpu.matmul_pop(refs[q // chunk % 2][q // chunk // 2])
            block = counts[q % chunk * n:(q % chunk + 1) * n]
            rank = jnp.sum(hot[q] * (block[:, :LANES] + base), axis=0, keepdims=True)
            base = base + block[:, LANES:]
            places[:, q * LANES:(q + 1) * LANES] = jnp.where(rank == slot, 1.0, 0.0).astype(jnp.bfloat16)
            fields.append(jnp.concatenate(
                [hot[q] * low[q:q + 1], hot[q] * high[q:q + 1], hot[q] * float(q)], axis=0
            ).astype(jnp.bfloat16))
        sums = (field0, field1)
        turns = owned // 4
        for i in range(turns):
            pairs = (2 * i, owned // 2 + 2 * i)
            pltpu.matmul_push_rhs(
                jnp.concatenate([places[:, q * LANES:(q + 2) * LANES] for q in pairs], axis=0),
                staging_register=i // 2 % 2, mxu_index=i % 2, transpose=True)
            pltpu.matmul_acc_lhs(
                sums[i % 2],
                jnp.concatenate([jnp.concatenate(fields[q:q + 2], axis=1) for q in pairs], axis=0),
                load_staged_rhs=i // 2 % 2)
        total = pltpu.matmul_pop(field0) + pltpu.matmul_pop(field1)
        sorted_fields = total[:3 * n, :LANES] + total[3 * n:, LANES:]
        packed = (
            sorted_fields[:n] + sorted_fields[n:2 * n] * float(LANES) + sorted_fields[2 * n:] * float(rows_dev)
        ).astype(jnp.int32)
        for t in range(n):
            ids_out[t] = packed[t:t + 1]
        ids_in[me] = ids_out[me]

    pl.run_scoped(
        sort,
        (pltpu.ACC(0)((TILE, TILE), jnp.float32),) * (owned * n // TILE // 2),
        (pltpu.ACC(1)((TILE, TILE), jnp.float32),) * (owned * n // TILE // 2),
        pltpu.ACC(0)((6 * n, TILE), jnp.float32),
        pltpu.ACC(1)((6 * n, TILE), jnp.float32))

    mark("sends2")
    for d in neighbours:
        send_ids(d)
    for k in range(1, tiles):
        @pl.when(my_tile >= k)
        def _():
            for d in plane_of(my_tile - k):
                send_ids(d)

    def reach_up(k):
        @pl.when(my_tile + k < tiles)
        def _():
            pl.semaphore_wait(in_sem.at[my_tile + k], 1)
            for d in plane_of(my_tile + k):
                send_ids(d)
            for d in same_core_of(my_tile + k):
                send_queries(d, q_recv.at[my_tile])

    def hand_over(p):
        blocks_of = q_in.at[pl.ds(core * chips + planes[p] * dpc, dpc)]
        bulk_wait(blocks_of, q_recv.at[planes[p]])
        pltpu.make_async_remote_copy(
            src_ref=blocks_of, dst_ref=blocks_of, send_sem=hand_send, recv_sem=hand_recv.at[planes[p]],
            device_id=(me + 1 - 2 * core), device_id_type=LOGICAL).start()

    left = lax.broadcasted_iota(jnp.int32, (owned, LANES), 1) < half

    def unpack(chip):
        f0 = q_in[chip].astype(jnp.float32)
        f1 = q_in[chips + chip].astype(jnp.float32)
        both = jnp.concatenate(
            [jnp.where(left, f0, pltpu.roll(f1, half, 1)), jnp.where(left, pltpu.roll(f0, half, 1), f1)], axis=0)
        q_full[pl.ds(pl.multiple_of(chip * 2 * owned, 2 * owned), 2 * owned), :] = both.astype(jnp.bfloat16)

    order = [(b // 2, b % 2) for b in range(2 * tiles)]

    def arrive(b):
        p, side = order[b]
        if b == 0:
            bulk_wait(q_in.at[pl.ds(0, dph - 1)], q_recv.at[tiles])
            first, many = my_tile * dpc + my_half * (dpc // 2), dpc // 2
        elif b == 1:
            bulk_wait(q_in.at[pl.ds(0, dph)], q_recv.at[tiles + 1])
            first, many = my_tile * dpc + (1 - my_half) * (dpc // 2), dpc // 2
        elif side == 0:
            bulk_wait(q_in.at[pl.ds(0, dpc)], hand_recv.at[planes[p]])
            first, many = planes[p] * dpc, dpc
        else:
            many = 0
        for g in range(many):
            unpack(first + g)

    def block_of(b):
        p, side = order[b]
        if b == 0:
            return my_tile * 2 + my_half
        if b == 1:
            return my_tile * 2 + 1 - my_half
        return planes[p] * 2 + side

    def stage_ids(u):
        @pl.when(my_tile == u)
        def _():
            bulk_wait(ids_in.at[pl.ds(0, dpt - 1)], ids_recv.at[askers[u]])

        @pl.when(my_tile != u)
        def _():
            bulk_wait(ids_in.at[pl.ds(0, dpt)], ids_recv.at[askers[u]])
        ids_at[pl.ds(u * dpt, dpt)] = jnp.bitwise_and(
            ids_in[pl.ds(pl.multiple_of(askers[u] * dpt, dpt), dpt)], jnp.int32(rows_dev - 1))
        to_smem(u).start()

    def to_smem(u):
        at = pl.ds(u * dpt, dpt)
        return pltpu.make_async_copy(ids_at.at[at], ids_sm.at[at], sm_sem.at[u])

    def send_vals(u):
        def send(at):
            pltpu.make_async_remote_copy(
                src_ref=vals_out.at[u * dpt + at], dst_ref=vals_in.at[me], send_sem=vals_send, recv_sem=vals_recv,
                device_id=(askers[u] * dpt + at), device_id_type=LOGICAL).start()

        for j in range(1, dpt):
            send((my_j + j) % dpt)

        @pl.when(my_tile != u)
        def _():
            send(my_j)

        @pl.when(my_tile == u)
        def _():
            vals_in[me] = vals_out[u * dpt + my_j]

    who_q = lax.broadcasted_iota(jnp.int32, (owned, LANES), 0)
    in_use = lax.broadcasted_iota(jnp.int32, (owned, LANES), 1) < capacity
    zeros = jnp.zeros((LANES, LANES), jnp.bfloat16)

    def diagonal(a, b):
        z = zeros[:a.shape[0]]
        return jnp.concatenate([jnp.concatenate([a, z], axis=1), jnp.concatenate([z, b], axis=1)], axis=0)

    def stream(*accs):
        ranges = (accs[:RANGES], accs[RANGES:2 * RANGES])
        extra = accs[2 * RANGES:]
        turn = [0, 0]
        staged = [[], []]
        pending = []
        sums = {}
        count = [0, 0]

        def push(m, value):
            r = turn[m]
            turn[m] = 1 - r
            pltpu.matmul_push_rhs(value, staging_register=r, mxu_index=m, transpose=True)
            staged[m].append(r)
            assert len(staged[m]) <= 2

        def weights(b):
            at = block_of(b)
            q = q_full[pl.ds(pl.multiple_of(at * LANES, LANES), LANES), :]
            return diagonal(q, q)

        def pop():
            kind, m, ref, data = pending.pop(0)
            got = pltpu.matmul_pop(ref)
            if kind == "sweep":
                over = jnp.maximum(got - data[1], 0.0).reshape(ROWS // 16, 2, 8, 2 * LANES)
                part = jnp.sum(over, axis=0)
                sums[data[0]] = sums[data[0]] + part if data[0] in sums else part
            else:
                u, a = data
                for e in range(2):
                    j = 2 * a + e
                    who = lax.shift_right_arithmetic(
                        ids_in[askers[u] * dpt + j], jnp.int32(id_bits))
                    picked = jnp.where((who == who_q) & in_use, got[:, e * LANES:(e + 1) * LANES], 0.0)
                    vals_out[u * dpt + j] = jnp.sum(picked, axis=0, keepdims=True)

        def drain(depth):
            while sum(kind == "sweep" for kind, *_ in pending) > depth:
                pop()
            if depth == 0:
                while pending:
                    pop()

        def finish(b):
            acc = sums.pop(b)
            acc = acc[0] + acc[1]
            acc = acc[:, :LANES] + acc[:, LANES:]
            at = block_of(b)
            mass_rows[b] = jnp.sum(acc, axis=0, keepdims=True)
            if b == 0:
                mass_in[me] = mass_rows[b]
                dests = own_half
            else:
                dests = [at * dph + j for j in around]
            for d in dests:
                pltpu.make_async_remote_copy(
                    src_ref=mass_rows.at[b], dst_ref=mass_in.at[me],
                    send_sem=mass_send, recv_sem=mass_recv,
                    device_id=(d), device_id_type=LOGICAL).start()

        def gather(u, k):
            j, r = k // capacity, k % capacity
            rows_v[u * dpt + j, pl.ds(r, 1), :] = corpus_f[pl.ds(ids_sm[u * dpt + j, 0, r], 1), :]

        def stage(b, m, pair):
            if pair is not None:
                at = pair[0] * dpt + 2 * pair[1]
                push(m, diagonal(rows_v[at].astype(jnp.bfloat16), rows_v[at + 1].astype(jnp.bfloat16)))
            push(m, weights(b))

        def reply(m, u, a, spare=0):
            ref = extra[m + 2 * spare]
            first = askers[u] * dpt + 2 * a
            q = q_full[pl.ds(pl.multiple_of(first * owned, 2 * owned), 2 * owned), :]
            pltpu.matmul_acc_lhs(
                ref, jnp.concatenate([q[:owned], q[owned:]], axis=1), load_staged_rhs=staged[m].pop(0))
            pending.append(("pair", m, ref, (u, a)))

        acts = dict(
            reach=reach_up, hand=hand_over, ids=stage_ids, sm=lambda u: to_smem(u).wait(), vals=send_vals,
            mass=finish, arrive=arrive)
        total = 2 * tiles * PIECES
        answers = {h + m: (u, 2 * k + m) for u in UNITS for k, h in enumerate(UNITS[u][2]) for m in range(2)}
        for step in range(total):
            b, piece, m = step // PIECES, step % PIECES, step % 2
            if step == 0:
                mark("arrive0")
                arrive(0)
                for side in range(2):
                    push(side, weights(0))
            for name, arg in PLAN.get(step, ()):
                mark(f"{name}{arg}")
                acts[name](arg)
            if step in PLAN or step == 0:
                mark(f"go{step}")
            if step in FENCES:
                pl.semaphore_signal(fence_sem, inc=1)
            if piece == 0:
                at = pl.ds(pl.multiple_of(block_of(b) * LANES, LANES), LANES)
                cut = thr_ref[:, at].astype(jnp.float32) * 0.01
                cut = jnp.concatenate([cut, cut], axis=1)
            if step in answers:
                reply(m, *answers[step])
            at = pl.ds(piece * ROWS, ROWS)
            lhs = jnp.concatenate(
                [corpus_v[at, :], corpus_v[pl.ds(rows_dev // 2 + piece * ROWS, ROWS), :]], axis=1)
            ref = ranges[m][count[m] % RANGES]
            count[m] += 1
            pltpu.matmul_acc_lhs(ref, lhs, load_staged_rhs=staged[m].pop(0) if staged[m] and step % 16 < 2 else None)
            pending.append(("sweep", m, ref, (b, cut)))
            for u, (s0, length, _) in UNITS.items():
                if s0 <= step < s0 + length:
                    for k in range((step - s0) * dpt * capacity // length, (step - s0 + 1) * dpt * capacity // length):
                        gather(u, k)
            ahead = step + AHEAD
            if ahead % 16 < 2 and 16 <= ahead < total and (ahead % PIECES < 2 or ahead in answers):
                stage(ahead // PIECES, ahead % 2, answers.get(ahead))
            drain(2 * LAG)
        drain(0)
        finish(2 * tiles - 1)

        mark("last")
        u = tiles - 1
        for k in range(dpt * capacity):
            gather(u, k)
        for a in range(dpt // 2):
            at = u * dpt + 2 * a
            push(a % 2, diagonal(rows_v[at].astype(jnp.bfloat16), rows_v[at + 1].astype(jnp.bfloat16)))
            reply(a % 2, u, a, a // 2)
        drain(0)
        send_vals(u)

    mark("reach1")
    reach_up(1)
    load.wait()
    mark("widen")

    def widen(b, carry):
        at = pl.ds(pl.multiple_of(b * WIDEN, WIDEN), WIDEN)
        corpus_f[at, :] = corpus_v[at, :].astype(jnp.float32)
        return carry
    lax.fori_loop(0, rows_dev // WIDEN, widen, 0)

    pl.run_scoped(
        stream,
        *[pltpu.ACC(0)((ROWS, TILE), jnp.float32)] * RANGES,
        *[pltpu.ACC(1)((ROWS, TILE), jnp.float32)] * RANGES,
        *[pltpu.ACC(m % 2)((owned, TILE), jnp.float32) for m in range(4)])

    mark("valswait")
    bulk_wait(vals_in.at[pl.ds(0, n - 1)], vals_recv)
    mark("spread")
    values = jnp.concatenate([vals_in[t] for t in range(n)], axis=0)
    top = values.astype(jnp.bfloat16)
    rest = values - top.astype(jnp.float32)
    mid = rest.astype(jnp.bfloat16)
    last = (rest - mid.astype(jnp.float32)).astype(jnp.bfloat16)
    upper_part = jnp.concatenate([top, mid], axis=1)
    lower_part = jnp.concatenate([last, jnp.zeros_like(last)], axis=1)
    cand = cand_pad[...]
    target = lax.shift_right_arithmetic(cand, jnp.int32(id_bits))
    dest = lax.broadcasted_iota(jnp.int32, (n, LANES), 0)

    def spread(*refs):
        for i in range(owned // 2):
            place = places[:, 2 * i * LANES:2 * (i + 1) * LANES]
            pltpu.matmul_push_rhs(
                jnp.concatenate([place, place], axis=0), staging_register=i // 2 % 2, mxu_index=i % 2)
            pltpu.matmul_acc_lhs(refs[i % 2][i // 2], upper_part, load_staged_rhs=i // 2 % 2)
            pltpu.matmul_acc_lhs(refs[i % 2][i // 2], lower_part)
        for i in range(owned // 2):
            both = pltpu.matmul_pop(refs[i % 2][i // 2])
            for e in range(2):
                q = 2 * i + e
                ans_out[q:q + 1, :] = jnp.sum(
                    jnp.where(target[q:q + 1] == dest, both[:, e * LANES:(e + 1) * LANES], 0.0),
                    axis=0, keepdims=True)[:, :per_query]

    pl.run_scoped(
        spread,
        (pltpu.ACC(0)((n, TILE), jnp.float32),) * (owned // 4),
        (pltpu.ACC(1)((n, TILE), jnp.float32),) * (owned // 4))

    mark("masswait")
    bulk_wait(mass_in.at[pl.ds(0, n - 1)], mass_recv)
    mark("masssum")
    mass = mass_in[0]
    for t in range(1, n):
        mass = mass + mass_in[t]
    mass = mass * (8.0 / npass_all)
    per_row = LANES // owned
    result = mass
    for u in range(1, per_row):
        result = jnp.where(me % per_row == u, pltpu.roll(mass, LANES - u * owned, 1), result)
    mass_out[...] = result[:, :owned]

    mark("sendwaits")
    pl.semaphore_wait(fence_sem, len(FENCES))
    bulk_wait(q_in.at[pl.ds(0, dpt - 1 + (tiles - 1) * dpc)], q_send)
    bulk_wait(q_in.at[pl.ds(0, (tiles - 1) * dpc)], hand_send)
    bulk_wait(ids_in.at[pl.ds(0, n - 1)], ids_send)
    bulk_wait(vals_in.at[pl.ds(0, n - 1)], vals_send)
    bulk_wait(mass_in.at[pl.ds(0, n - 1)], mass_send)
    mark(None)


def fused_body(n, nf, queries, corpus, candidates, threshold):
    rows_dev, width = corpus.shape
    owned, per_query = candidates.shape
    nq = n * owned
    tiles = nq // TILE
    capacity = (owned * per_query + n - 1) // n
    mass, answers = pl.pallas_call(
        functools.partial(kernel, n, nf, rows_dev * n, capacity),
        out_shape=(
            pltpu.VMEM((1, owned), jnp.float32),
            pltpu.VMEM((owned, per_query), jnp.float32),
        ),
        in_specs=[pl.BlockSpec(memory_space=pl.ANY)] * 4,
        out_specs=[pl.BlockSpec(memory_space=pltpu.VMEM)] * 2,
        scratch_shapes=[
            pltpu.VMEM(queries.shape, jnp.bfloat16),
            pltpu.VMEM((1, nq), jnp.int32),
            pltpu.VMEM((owned, per_query), jnp.int32),
            pltpu.VMEM((rows_dev, width), jnp.bfloat16),
            pltpu.VMEM((rows_dev, width), jnp.float32),
            pltpu.VMEM((owned, LANES), jnp.bfloat16),
            pltpu.VMEM((n, owned, LANES), jnp.bfloat16),
            pltpu.VMEM((nq, LANES), jnp.bfloat16),
            pltpu.VMEM((owned, LANES), jnp.int32),
            pltpu.VMEM((LANES, owned * LANES), jnp.bfloat16),
            pltpu.VMEM((n, 1, LANES), jnp.int32),
            pltpu.VMEM((n, 1, LANES), jnp.int32),
            pltpu.VMEM((n, 1, LANES), jnp.int32),
            pltpu.SMEM((n, 1, LANES), jnp.int32),
            pltpu.VMEM((n, LANES, LANES), jnp.float32),
            pltpu.VMEM((n, 1, LANES), jnp.float32),
            pltpu.VMEM((n, 1, LANES), jnp.float32),
            pltpu.VMEM((nq // LANES, 1, LANES), jnp.float32),
            pltpu.VMEM((n, 1, LANES), jnp.float32),
            pltpu.SemaphoreType.DMA((3,)),
            pltpu.SemaphoreType.DMA,
            pltpu.SemaphoreType.DMA((tiles,)),
            pltpu.SemaphoreType.REGULAR((tiles,)),
            pltpu.SemaphoreType.REGULAR,
            pltpu.SemaphoreType.DMA,
            pltpu.SemaphoreType.DMA((tiles + 2,)),
            pltpu.SemaphoreType.DMA,
            pltpu.SemaphoreType.DMA((tiles,)),
            pltpu.SemaphoreType.DMA,
            pltpu.SemaphoreType.DMA((tiles,)),
            pltpu.SemaphoreType.DMA,
            pltpu.SemaphoreType.DMA,
            pltpu.SemaphoreType.DMA,
            pltpu.SemaphoreType.DMA,
        ],
        compiler_params=pltpu.CompilerParams(
            collective_id=0, has_side_effects=True),
    )(queries, threshold.reshape(1, nq), candidates, corpus)
    return mass.reshape(owned), answers


def plain_body(queries, corpus, candidates, threshold):
    rows_dev = corpus.shape[0]
    width = corpus.shape[1]
    shards = lax.axis_size("rows") * lax.axis_size("feat")
    owned_queries = candidates.shape[0]
    per_query = candidates.shape[1]
    npass_all = rows_dev * shards
    cutoff = threshold.astype(jnp.float32) * 0.01
    owner = lax.axis_index(("rows", "feat"))
    full_rows = lax.all_gather(queries, "feat", axis=1, tiled=True)
    whole = lax.all_gather(full_rows, "rows", axis=0, tiled=True)
    query_count = whole.shape[0]
    block = 2048
    corpus_blocks = corpus.reshape(rows_dev // block, block, width)

    def visit(total, block_rows):
        scores = lax.dot_general(
            whole, block_rows, (((1,), (1,)), ((), ())), preferred_element_type=jnp.float32
        )
        return (total + jnp.sum(jnp.maximum(scores - cutoff[:, None], 0.0), axis=1), None)

    total, _ = lax.scan(visit, jnp.zeros((query_count,), jnp.float32), corpus_blocks)
    flat_ids = candidates.reshape(-1)
    total_ids = flat_ids.shape[0]
    capacity = (total_ids + shards - 1) // shards
    target = flat_ids // rows_dev
    onehot = (target[:, None] == jnp.arange(shards, dtype=jnp.int32)[None, :]).astype(jnp.int32)
    before = jnp.cumsum(onehot, axis=0) - onehot
    rank = jnp.sum(before * onehot, axis=1)
    query_ids = owner * owned_queries + jnp.arange(total_ids, dtype=jnp.int32) // per_query
    fields = jnp.stack([flat_ids - target * rows_dev, query_ids], axis=1)
    send_both = jnp.zeros((shards, capacity, 2), jnp.int32).at[target, rank].set(fields)
    n_rows = lax.axis_size("rows")
    n_feat = lax.axis_size("feat")
    received = lax.all_to_all(
        lax.all_to_all(
            send_both.reshape(n_rows, n_feat, capacity * 2),
            "rows",
            split_axis=0,
            concat_axis=0,
            tiled=True,
        ),
        "feat",
        split_axis=1,
        concat_axis=1,
        tiled=True,
    )
    received = received.reshape(shards * capacity, 2)
    picked = corpus[received[:, 0]]
    asked = whole[received[:, 1]]
    values = jnp.einsum("kd,kd->k", picked, asked, preferred_element_type=jnp.float32).reshape(
        n_rows, n_feat, capacity
    )
    partials = total.reshape(n_rows, n_feat, owned_queries)
    answers, mass_parts = (
        lax.all_to_all(
            lax.all_to_all(values, "rows", split_axis=0, concat_axis=0, tiled=True),
            "feat",
            split_axis=1,
            concat_axis=1,
            tiled=True,
        ),
        lax.all_to_all(
            lax.all_to_all(partials, "rows", split_axis=0, concat_axis=0, tiled=True),
            "feat",
            split_axis=1,
            concat_axis=1,
            tiled=True,
        ),
    )
    exceed = jnp.sum(mass_parts, axis=(0, 1)) * (8.0 / npass_all)
    candidate_scores = answers.reshape(shards, capacity)[target, rank].reshape(
        owned_queries, per_query
    )
    return (exceed, candidate_scores)


def body(queries, corpus, candidates, threshold):
    nf = lax.axis_size("feat")
    n = lax.axis_size("rows") * nf
    rows_dev, width = corpus.shape
    owned, per_query = candidates.shape
    capacity = (owned * per_query + n - 1) // n
    fits = (
        nf == 2
        and width == LANES
        and queries.shape == (2 * owned, LANES // 2)
        and owned % 32 == 0
        and LANES % owned == 0
        and per_query <= LANES
        and capacity <= LANES
        and n % 8 == 0
        and (n * owned) % TILE == 0
        and n * owned == 4 * TILE
        and rows_dev == 2 * ROWS * PIECES
        and rows_dev & (rows_dev - 1) == 0
    )
    if fits:
        return fused_body(n, nf, queries, corpus, candidates, threshold)
    return plain_body(queries, corpus, candidates, threshold)


def solution(mesh):
    return jax.shard_map(
        body,
        mesh=mesh,
        in_specs=(P("rows", "feat"), P(("rows", "feat"), None), P(("rows", "feat"), None), P()),
        out_specs=(P(("rows", "feat")), P(("rows", "feat"), None)),
        check_vma=False,
    )
```
